512 devices in a mesh: row: 16 (over z_hi, x, core), col: 32 (over y, z_lo).
Axes of the slice: x: 4, y: 4, z: 16 (z_hi: 2, z_lo: 8; z = z_hi * 8 + z_lo), core: 2. Of those that a mesh axis runs over, the one named last changes fastest.
Arguments:
- geometry: float32 [4, 786432], P(None, ('row', 'col')), may hold values from -1 to 1, as said below
- charges: bfloat16 [32, 786432], P(None, ('row', 'col')), may hold values from -6 to 6
- near_index: int32 [6144, 128], P(('row', 'col')), may hold values from 0 to 4607
- near_count: int32 [6144], P(('row', 'col')), may hold values from 1 to 128
- near_weight: bfloat16 [6144, 128, 128], P(('row', 'col')), may hold values from -0.5 to 0.5
- conductor: int32 [786432], P(('row', 'col')), may hold values from 0 to 31
Outputs:
- potential: float32 [32, 786432], P(None, ('row', 'col'))
- conductor_totals: float32 [32, 32], replicated
The draws below stay inside these ranges and needn't reach their ends.
Inputs may be any that keep to these rules, and one draw needn't show every extreme that they name: `geometry`: rows 0 to 2 are coordinates in [-1, 1]; row 3 is a panel size in [0.05, 0.2].
All inputs are finite; a program needn't handle non-finite values.
Results may differ from the reference program's by a relative error of at most 0.0044.
Values may be sent and summed in bfloat16 or wider, within the bound.
A program may use at most 64 MiB of HBM per device.

```python
import jax
import jax.numpy as jnp
from jax import lax

BLOCK = 1536
RHS = 32
ROUNDS = 8
GROUP = 128
NEAR = 128
PANELS = 786432
GROUPS = 6144


def draw_geometry(key, part):
    place_key = jax.random.fold_in(key, 11)
    size_key = jax.random.fold_in(key, 12)
    coords = jax.random.uniform(place_key, (3, PANELS), jnp.float32, -1.0, 1.0)
    sizes = jnp.exp(jax.random.uniform(size_key, (1, PANELS), jnp.float32, jnp.log(0.05), jnp.log(0.2)))
    return jnp.concatenate([coords, sizes], axis=0).astype(jnp.float32)


def place_ends(drawn, key, least, top_value):
    place = [jax.random.randint(jax.random.fold_in(key, axis), (), 0, length) for axis, length in enumerate(drawn.shape)]
    main_axis = drawn.shape.index(max(drawn.shape))
    next_to = place[:main_axis] + [(place[main_axis] + 1) % drawn.shape[main_axis]] + place[main_axis + 1:]
    return drawn.at[tuple(place)].set(least).at[tuple(next_to)].set(top_value)


def level_of(stream_key, extent, split, smallest, high):
    def one(dim, blocks):
        steps = jax.random.uniform(jax.random.fold_in(jax.random.fold_in(stream_key, 6), dim), (blocks,), jnp.float32, smallest / len(split), high / len(split))
        return jnp.repeat(jnp.exp(steps), extent[dim] // blocks).reshape((-1,) + (1,) * (len(extent) - dim - 1))

    loudness = one(*split[0])
    for cut in split[1:]:
        loudness = loudness * one(*cut)
    return loudness


def bell_draw(rng, extent, deviation, limit, pieces=(), kind=jnp.bfloat16):
    values = deviation * jax.random.normal(rng, extent, jnp.float32)
    if pieces:
        values = values * level_of(rng, extent, pieces, -0.22, 0.18)
    return jnp.clip(values, -limit, limit).astype(kind)


def setup_inputs(seed: int = 0) -> dict:
    key_list = jax.random.split(jax.random.key(seed), 7)
    geometry = draw_geometry(jax.random.fold_in(key_list[6], 71), 0)
    charges = bell_draw(key_list[1], (RHS, PANELS), 1.0, 6.0, ((1, 512),))
    near_index = place_ends(jax.random.randint(key_list[2], (GROUPS, NEAR), 0, 3 * BLOCK), jax.random.fold_in(key_list[2], 1), 0, (3 * BLOCK) - 1).astype(jnp.int32)
    near_count = place_ends(jax.random.randint(key_list[3], (GROUPS,), 1, NEAR + 1), jax.random.fold_in(key_list[3], 1), 1, NEAR).astype(jnp.int32)
    near_weight = bell_draw(key_list[4], (GROUPS, GROUP, NEAR), NEAR ** -0.5, 0.5, ((0, 512),))
    conductor = place_ends(jax.random.randint(key_list[5], (PANELS,), 0, RHS), jax.random.fold_in(key_list[5], 1), 0, RHS - 1).astype(jnp.int32)
    return {"geometry": geometry, "charges": charges, "near_index": near_index, "near_count": near_count, "near_weight": near_weight, "conductor": conductor}


def kernel_tile(rows, cols):
    delta_x = rows[0][:, None] - cols[0][None, :]
    delta_y = rows[1][:, None] - cols[1][None, :]
    delta_z = rows[2][:, None] - cols[2][None, :]
    spread = rows[3][:, None] * rows[3][:, None] + cols[3][None, :] * cols[3][None, :]
    squared = delta_x * delta_x + delta_y * delta_y + delta_z * delta_z + spread
    return lax.rsqrt(squared).astype(jnp.bfloat16)

def reference(geometry, charges, near_index, near_count, near_weight, conductor):
    blocks = PANELS // BLOCK
    stride = blocks // (2 * ROUNDS)
    offsets = [1 + k * stride for k in range(ROUNDS)]
    groups_dev = BLOCK // GROUP
    area = geometry[3] * geometry[3]
    weighted = (charges.astype(jnp.float32) * area[None, :]).astype(jnp.bfloat16)

    def piece(array, block):
        return lax.dynamic_slice_in_dim(array, (block * BLOCK).astype(jnp.int32), BLOCK, 1)

    def visit(field, block):
        own_geo = piece(geometry, block)
        own_w = piece(weighted, block)
        tile = kernel_tile(own_geo, own_geo)
        forward = lax.dot_general(own_w, tile, (((1,), (1,)), ((), ())), preferred_element_type=jnp.float32)
        for offset in offsets:
            other = ((block - offset) % blocks).astype(jnp.int32)
            tile = kernel_tile(own_geo, piece(geometry, other))
            forward = forward + lax.dot_general(piece(weighted, other), tile, (((1,), (1,)), ((), ())), preferred_element_type=jnp.float32)
            back = jnp.dot(own_w, tile, preferred_element_type=jnp.float32).astype(jnp.bfloat16).astype(jnp.float32)
            start = (other * BLOCK).astype(jnp.int32)
            current = lax.dynamic_slice_in_dim(field, start, BLOCK, 1)
            field = lax.dynamic_update_slice_in_dim(field, current + back, start, 1)
        lower = ((block - 1) % blocks).astype(jnp.int32)
        upper = ((block + 1) % blocks).astype(jnp.int32)
        extended = jnp.concatenate([piece(charges, lower), piece(charges, block), piece(charges, upper)], axis=1)
        first = (block * groups_dev).astype(jnp.int32)
        indices = lax.dynamic_slice_in_dim(near_index, first, groups_dev, 0)
        counts = lax.dynamic_slice_in_dim(near_count, first, groups_dev, 0)
        weights = lax.dynamic_slice_in_dim(near_weight, first, groups_dev, 0)
        gathered = jnp.take(extended, indices.reshape(-1), axis=1).reshape(RHS, groups_dev, NEAR)
        live = jnp.arange(NEAR, dtype=jnp.int32)[None, :] < counts[:, None]
        gathered = jnp.where(live[None], gathered, jnp.zeros_like(gathered))
        correction = jnp.einsum('rgk,gtk->rgt', gathered.astype(jnp.float32), weights.astype(jnp.float32)).reshape(RHS, BLOCK)
        start = (block * BLOCK).astype(jnp.int32)
        current = lax.dynamic_slice_in_dim(field, start, BLOCK, 1)
        field = lax.dynamic_update_slice_in_dim(field, current + forward + correction, start, 1)
        return (field, None)
    field = jnp.zeros((RHS, PANELS), jnp.float32)
    field, _ = lax.scan(visit, field, jnp.arange(blocks, dtype=jnp.int32))
    scaled = (field * area[None, :]).T
    totals = jax.ops.segment_sum(scaled, conductor, num_segments=RHS).T
    return (field, totals)
```

```python
import functools

import jax
import jax.numpy as jnp
from jax import lax
from jax.experimental import pallas as pl
from jax.experimental.pallas import tpu as pltpu
from jax.sharding import PartitionSpec as P

MESH = pl.DeviceIdType.MESH
BLOCK = 1536
RHS = 32
GROUPS = 12
ROWBLK = 256
ROWS = 16
COLS = 32
F32 = jnp.float32
BF16 = jnp.bfloat16
VMEM = pl.BlockSpec(memory_space=pltpu.VMEM)
SMEM = pl.BlockSpec(memory_space=pltpu.SMEM)
NT = (((1,), (1,)), ((), ()))


def three(v):
    high = v.astype(BF16).astype(F32)
    rest = v - high
    mid = rest.astype(BF16).astype(F32)
    return high, mid, rest - mid


def features(geo):
    high, mid, low = three(geo[0:3])
    norm = (
        geo[0:1] * geo[0:1] + geo[1:2] * geo[1:2] + geo[2:3] * geo[2:3] + geo[3:4] * geo[3:4]
    )
    nh, nm, nl = three(norm)
    one = jnp.ones_like(norm)
    pad = jnp.zeros((7, geo.shape[1]), F32)
    left = [high, high, high, mid, mid, mid, low, low, low, nh, nm, nl, one, one, one, pad]
    h2, m2, l2 = -2.0 * high, -2.0 * mid, -2.0 * low
    right = [h2, m2, l2, h2, m2, l2, h2, m2, l2, one, one, one, nh, nm, nl, pad]
    return left, right


def shifted(row, col, steps):
    flat = lax.rem(row * COLS + col + (steps + 2 * ROWS * COLS), ROWS * COLS)
    return flat // COLS, lax.rem(flat, COLS)


def potential_kernel(
    geo_ref, chg_ref, ni_ref, nc_ref, nw_ref, cond_ref, pot_ref, tot_ref,
    feat, right, wown, woth, back, acc_u, acc_v, tile_a, tile_b,
    ug, uc, vg, vc, ac, xg, xc, sb, rb, su, sv, ru, rv,
    send_u, recv_u, send_v, recv_v, send_a, recv_a, send_x, recv_x, send_b, recv_b, send_r, recv_r,
):
    row = lax.axis_index("row")
    col = lax.axis_index("col")
    place = lax.rem(row, 8)
    base = row - place
    up1 = shifted(row, col, 1)
    down1 = shifted(row, col, -1)
    up257 = shifted(row, col, 257)
    down257 = shifted(row, col, -257)
    sends_v = lax.rem(up257[0], 8) != 0
    takes_v = place != 0

    def mate(step):
        return base + lax.rem(place + step, 8), col

    barrier = pltpu.get_barrier_semaphore()
    for other in (up1, down1, up257, down257):
        pl.semaphore_signal(barrier, inc=1, device_id=other, device_id_type=MESH)
    for step in range(1, 8):
        pl.semaphore_signal(barrier, inc=1, device_id=mate(step), device_id_type=MESH)

    def remote(src, dst, ssem, rsem, where):
        return pltpu.make_async_remote_copy(
            src_ref=src, dst_ref=dst, send_sem=ssem, recv_sem=rsem, device_id=where,
            device_id_type=MESH,
        )

    copies_u = [
        remote(geo_ref, ug, send_u.at[0], recv_u.at[0], up1),
        remote(chg_ref, uc, send_u.at[1], recv_u.at[1], up1),
    ]
    copies_v = [
        remote(geo_ref, vg, send_v.at[0], recv_v.at[0], up257),
        remote(chg_ref, vc, send_v.at[1], recv_v.at[1], up257),
    ]
    copy_a = remote(chg_ref, ac, send_a, recv_a, down1)

    def group_copies(step, geo, chg):
        return [
            remote(geo, xg.at[step], send_x.at[0, step], recv_x.at[0, step], mate(step)),
            remote(chg, xc.at[step], send_x.at[1, step], recv_x.at[1, step], mate(step)),
        ]

    def back_copy(step):
        return remote(sb.at[step], rb.at[step], send_b.at[step], recv_b.at[step], mate(8 - step))

    copy_ru = remote(su, ru, send_r.at[0], recv_r.at[0], down1)
    copy_rv = remote(sv, rv, send_r.at[1], recv_r.at[1], down257)

    own = geo_ref[...]
    feat[...] = jnp.concatenate(features(own)[0], axis=0).T.astype(BF16)
    wown[...] = (chg_ref[...].astype(F32) * (own[3:4] * own[3:4])).astype(BF16)
    pot_ref[...] = jnp.zeros_like(pot_ref)

    def visit(geo, chg):
        right[...] = jnp.concatenate(features(geo)[1], axis=0).astype(BF16)
        woth[...] = (chg.astype(F32) * (geo[3:4] * geo[3:4])).astype(BF16)
        back[...] = jnp.zeros_like(back)
        tiles = (tile_a, tile_b)

        def fill(r):
            squared = jnp.dot(
                feat[r * ROWBLK : (r + 1) * ROWBLK, :], right[...], preferred_element_type=F32
            )
            tiles[r % 2][...] = lax.rsqrt(squared).astype(BF16)

        fill(0)
        for r in range(BLOCK // ROWBLK):
            if r + 1 < BLOCK // ROWBLK:
                fill(r + 1)
            rows = slice(r * ROWBLK, (r + 1) * ROWBLK)
            tile = tiles[r % 2][...]
            pot_ref[:, rows] += lax.dot_general(woth[...], tile, NT, preferred_element_type=F32)
            back[...] += jnp.dot(wown[:, rows], tile, preferred_element_type=F32)

    visit(own, chg_ref[...])

    pl.semaphore_wait(barrier, 11)

    @pl.when(sends_v)
    def _():
        for copy in copies_v:
            copy.start()

    for copy in copies_u:
        copy.start()
    copy_a.start()

    for copy in copies_u:
        copy.wait_recv()
    for step in range(1, 8):

        @pl.when(place + step < 8)
        def _():
            for copy in group_copies(step, ug, uc):
                copy.start()

    visit(ug[...], uc[...])
    acc_u[...] = back[...]
    acc_v[...] = jnp.zeros_like(acc_v)

    copy_a.wait_recv()

    def near(g, carry):
        index = ni_ref[pl.ds(g, 1), :]
        lane = lax.broadcasted_iota(jnp.int32, (1, 128), 1)
        index = jnp.where(lane < nc_ref[g], index, -1)
        slot = lax.broadcasted_iota(jnp.int32, (BLOCK, 128), 0)
        taken = jnp.zeros((RHS, 128), F32)
        for part, ref in enumerate((uc, chg_ref, ac)):
            pick = jnp.where(slot == index - part * BLOCK, 1.0, 0.0).astype(BF16)
            taken = taken + jnp.dot(ref[...], pick, preferred_element_type=F32)
        columns = pl.ds(pl.multiple_of(g * 128, 128), 128)
        pot_ref[:, columns] += lax.dot_general(
            taken.astype(BF16), nw_ref[g], NT, preferred_element_type=F32
        )
        return carry

    lax.fori_loop(0, GROUPS, near, 0)

    def round_(step, carry):
        @pl.when((step == jnp.minimum(place + 1, 4)) & takes_v)
        def _():
            for copy in copies_v:
                copy.wait_recv()
            for other in range(1, 8):

                @pl.when(place + other >= 8)
                def _():
                    for copy in group_copies(other, vg, vc):
                        copy.start()

        for copy in group_copies(step, ug, uc):
            copy.wait_recv()
        visit(xg[step], xc[step])
        sb[step] = back[...].astype(BF16)
        back_copy(step).start()
        return carry

    lax.fori_loop(1, 8, round_, 0)

    def collect(step, carry):
        back_copy(step).wait_recv()
        got = rb[step].astype(F32)

        @pl.when(place + step < 8)
        def _():
            acc_u[...] += got

        @pl.when(place + step >= 8)
        def _():
            acc_v[...] += got

        return carry

    lax.fori_loop(1, 8, collect, 0)
    sv[...] = acc_v[...].astype(BF16)
    su[...] = acc_u[...].astype(BF16)

    @pl.when(takes_v)
    def _():
        copy_rv.start()

    copy_ru.start()
    copy_ru.wait_recv()
    pot_ref[...] += ru[...].astype(F32)

    @pl.when(sends_v)
    def _():
        copy_rv.wait_recv()
        pot_ref[...] += rv[...].astype(F32)

    scaled = pot_ref[...] * (own[3:4] * own[3:4])
    pieces = three(scaled)
    slot = lax.broadcasted_iota(jnp.int32, (128, BLOCK), 0)
    total = jnp.zeros((8, 128), F32)
    for quarter in range(4):
        member = jnp.where(slot == cond_ref[...] + RHS * quarter, 1.0, 0.0).astype(BF16)
        for piece in pieces:
            part = piece[quarter * 8 : quarter * 8 + 8].astype(BF16)
            total = total + lax.dot_general(part, member, NT, preferred_element_type=F32)
    tot_ref[...] = total

    for copy in copies_u:
        copy.wait_send()
    copy_a.wait_send()

    @pl.when(sends_v)
    def _():
        for copy in copies_v:
            copy.wait_send()

    @pl.when(takes_v)
    def _():
        copy_rv.wait_send()

    copy_ru.wait_send()

    def drain(step, carry):
        for copy in group_copies(step, ug, uc):
            copy.wait_send()
        back_copy(step).wait_send()
        return carry

    lax.fori_loop(1, 8, drain, 0)


def totals_kernel(local_ref, out_ref, s1, s2, s3, send, recv1, recv2, recv3):
    row = lax.axis_index("row")
    col = lax.axis_index("col")
    place = lax.rem(row, 8)
    zhigh = row // 8
    yplace = col // 8
    zlow = lax.rem(col, 8)
    zplace = zhigh * 8 + zlow

    def in_group(step):
        return zhigh * 8 + lax.rem(place + step, 8), col

    def in_y(step):
        return row, lax.rem(yplace + step, 4) * 8 + zlow

    def in_z(step):
        other = lax.rem(zplace + step, 16)
        return (other // 8) * 8 + place, yplace * 8 + lax.rem(other, 8)

    stages = (
        (8, place, in_group, s1, recv1),
        (4, yplace, in_y, s2, recv2),
        (16, zplace, in_z, s3, recv3),
    )
    barrier = pltpu.get_barrier_semaphore()
    for count, _, where, _, _ in stages:
        for step in range(1, count):
            pl.semaphore_signal(barrier, inc=1, device_id=where(step), device_id_type=MESH)
    pl.semaphore_wait(barrier, 25)

    value = local_ref[...]
    sent = 0
    copies = []
    for count, mine, where, slots, recv in stages:
        slots[mine] = value
        stage = []
        for step in range(1, count):
            stage.append(
                pltpu.make_async_remote_copy(
                    src_ref=slots.at[mine], dst_ref=slots.at[mine], send_sem=send.at[sent],
                    recv_sem=recv.at[step], device_id=where(step), device_id_type=MESH,
                )
            )
            sent += 1
        for copy in stage:
            copy.start()
        for copy in stage:
            copy.wait_recv()
        value = slots[0]
        for other in range(1, count):
            value = value + slots[other]
        copies += stage
    out_ref[...] = value
    for copy in copies:
        copy.wait_send()


def on_device(geometry, charges, near_index, near_count, near_weight, conductor):
    def slots(*shape):
        return pltpu.VMEM(shape, BF16)

    dma = pltpu.SemaphoreType.DMA
    potential, local = pl.pallas_call(
        potential_kernel,
        out_shape=(
            jax.ShapeDtypeStruct((RHS, BLOCK), F32),
            jax.ShapeDtypeStruct((8, 128), F32),
        ),
        in_specs=[VMEM, VMEM, VMEM, SMEM, VMEM, VMEM],
        out_specs=(VMEM, VMEM),
        scratch_shapes=[
            slots(BLOCK, 40), slots(40, BLOCK), slots(RHS, BLOCK), slots(RHS, BLOCK),
            pltpu.VMEM((RHS, BLOCK), F32), pltpu.VMEM((RHS, BLOCK), F32),
            pltpu.VMEM((RHS, BLOCK), F32), slots(ROWBLK, BLOCK), slots(ROWBLK, BLOCK),
            pltpu.VMEM((4, BLOCK), F32), slots(RHS, BLOCK), pltpu.VMEM((4, BLOCK), F32),
            slots(RHS, BLOCK), slots(RHS, BLOCK), pltpu.VMEM((8, 4, BLOCK), F32),
            slots(8, RHS, BLOCK), slots(8, RHS, BLOCK), slots(8, RHS, BLOCK),
            slots(RHS, BLOCK), slots(RHS, BLOCK), slots(RHS, BLOCK), slots(RHS, BLOCK),
            dma((2,)), dma((2,)), dma((2,)), dma((2,)), dma, dma, dma((2, 8)), dma((2, 8)),
            dma((8,)), dma((8,)), dma((2,)), dma((2,)),
        ],
        compiler_params=pltpu.CompilerParams(
            collective_id=0, has_side_effects=True, vmem_limit_bytes=48 * 2**20
        ),
        name="potential",
    )(geometry, charges, near_index, near_count, near_weight, conductor.reshape(1, BLOCK))
    packed = pl.pallas_call(
        totals_kernel,
        out_shape=jax.ShapeDtypeStruct((8, 128), F32),
        in_specs=[VMEM],
        out_specs=VMEM,
        scratch_shapes=[
            pltpu.VMEM((8, 8, 128), F32), pltpu.VMEM((4, 8, 128), F32),
            pltpu.VMEM((16, 8, 128), F32), dma((25,)), dma((8,)), dma((4,)), dma((16,)),
        ],
        compiler_params=pltpu.CompilerParams(collective_id=1, has_side_effects=True),
        name="totals",
    )(local)
    totals = packed.reshape(8, 4, RHS).transpose(1, 0, 2).reshape(RHS, RHS)
    return potential, totals


def solution(mesh):
    in_specs = (
        P(None, ("row", "col")),
        P(None, ("row", "col")),
        P(("row", "col"), None),
        P(("row", "col")),
        P(("row", "col"), None, None),
        P(("row", "col")),
    )
    out_specs = (P(None, ("row", "col")), P())
    return jax.shard_map(
        on_device, mesh=mesh, in_specs=in_specs, out_specs=out_specs, check_vma=False
    )
```

```python
import jax
import jax.numpy as jnp
from jax import lax
from jax.experimental import pallas as pl
from jax.experimental.pallas import tpu as pltpu
from jax.sharding import PartitionSpec as P

MESH = pl.DeviceIdType.MESH
BLOCK = 1536
HALVES = 2
HALF = BLOCK // HALVES
RHS = 32
GROUPS = 12
ROWBLK = 256
ROWS = 16
COLS = 32
SEND_FIRST = 4
SEND_SECOND = 7
F32 = jnp.float32
BF16 = jnp.bfloat16
VMEM = pl.BlockSpec(memory_space=pltpu.VMEM)
SMEM = pl.BlockSpec(memory_space=pltpu.SMEM)
HBM = pl.BlockSpec(memory_space=pltpu.HBM)
NT = (((1,), (1,)), ((), ()))


def three(v):
    high = v.astype(BF16).astype(F32)
    rest = v - high
    mid = rest.astype(BF16).astype(F32)
    return high, mid, rest - mid


def features(geo):
    high, mid, low = three(geo[0:3])
    norm = (
        geo[0:1] * geo[0:1] + geo[1:2] * geo[1:2] + geo[2:3] * geo[2:3] + geo[3:4] * geo[3:4]
    )
    nh, nm, nl = three(norm)
    one = jnp.ones_like(norm)
    pad = jnp.zeros((7, geo.shape[1]), F32)
    left = [high, high, high, mid, mid, mid, low, low, low, nh, nm, nl, one, one, one, pad]
    h2, m2, l2 = -2.0 * high, -2.0 * mid, -2.0 * low
    right = [h2, m2, l2, h2, m2, l2, h2, m2, l2, one, one, one, nh, nm, nl, pad]
    return left, right


def shifted(row, col, steps):
    flat = lax.rem(row * COLS + col + (steps + 2 * ROWS * COLS), ROWS * COLS)
    return flat // COLS, lax.rem(flat, COLS)


def member_totals(value, size, conductor):
    pieces = three(value * (size * size))
    slot = lax.broadcasted_iota(jnp.int32, (RHS, value.shape[1]), 0)
    member = jnp.where(slot == conductor, 1.0, 0.0).astype(BF16)
    total = jnp.zeros((RHS, RHS), F32)
    for piece in pieces:
        total = total + lax.dot_general(
            piece.astype(BF16), member, NT, preferred_element_type=F32
        )
    return total


def kernel(
    geo_in, chg_in, ni_in, nc_ref, nw_in, cond_in, pot_ref, tot_ref,
    geo, chg, ni, nw, cond, in_sem,
    feat, right, wown, woth, back, acc_w, keep, total, tile_a, tile_b,
    xg, xc, xk, ac, sp, sq, pb, rb, sy, ry, sh, rh, s1, s2, s3,
    send_w, recv_w, send_y, recv_y, send_a, recv_a, send_x, recv_x, send_p, recv_p,
    send_b, recv_b, send_m, recv_m, send_h, recv_h, send_t, recv1, recv2, recv3,
):
    row = lax.axis_index("row")
    col = lax.axis_index("col")
    zhigh = row // 8
    place = lax.rem(row, 8)
    chip = place // 2
    core = lax.rem(place, 2)
    yplace = col // 8
    zlow = lax.rem(col, 8)
    zplace = zhigh * 8 + zlow
    up1 = shifted(row, col, 1)
    down1 = shifted(row, col, -1)
    near_dst = shifted(row, col, jnp.where(zlow == 7, 257, 1))
    near_src = shifted(row, col, jnp.where(zlow == 0, -257, -1))
    mate = (lax.rem(row + 8, ROWS), col)
    partner = (zhigh * 8 + chip * 2 + 1 - core, col)
    near_up = zlow != 0
    near_flag = near_up.astype(jnp.int32)
    far = jnp.logical_not(near_up & (place == 0))
    upper_slot = 8 - near_flag
    early = jnp.where(near_up, place + 1, 7 - place)
    late = 8 - early
    lead = jnp.where(near_up, core, 1 - core)
    near_field_early = near_up & (zlow != 7)

    def peer(step):
        return zhigh * 8 + lax.rem(chip + step, 4) * 2 + core, col

    def in_group(step):
        return zhigh * 8 + lax.rem(place + step, 8), col

    def in_y(step):
        return row, lax.rem(yplace + step, 4) * 8 + zlow

    def in_z(step):
        other = lax.rem(zplace + step, 16)
        return (other // 8) * 8 + place, yplace * 8 + lax.rem(other, 8)

    barrier = pltpu.get_barrier_semaphore()
    for other in (mate, near_dst, near_src, up1, down1):
        pl.semaphore_signal(barrier, inc=1, device_id=other, device_id_type=MESH)
    for count, where in ((16, in_z), (4, in_y), (8, in_group)):
        for step in range(1, count):
            pl.semaphore_signal(barrier, inc=1, device_id=where(step), device_id_type=MESH)

    loads = [
        pltpu.make_async_copy(src, dst, in_sem.at[i])
        for i, (src, dst) in enumerate(
            ((geo_in, geo), (chg_in, chg), (ni_in, ni), (nw_in, nw), (cond_in, cond))
        )
    ]
    for load in loads:
        load.start()

    def remote(src, dst, ssem, rsem, where):
        return pltpu.make_async_remote_copy(
            src_ref=src, dst_ref=dst, send_sem=ssem, recv_sem=rsem, device_id=where,
            device_id_type=MESH,
        )

    def w_copies(half):
        lanes = pl.ds(half * HALF, HALF)
        return [
            remote(
                src.at[:, lanes], dst.at[half], send_w.at[i, half], recv_w.at[i, half], near_dst
            )
            for i, (src, dst) in enumerate(
                zip((geo, chg, cond), (xg.at[7], xc.at[7], xk.at[0]))
            )
        ]

    def y_copies(half):
        return [
            remote(
                ref.at[src, half], ref.at[dst, half], send_y.at[i, half], recv_y.at[i, half], mate
            )
            for i, (ref, src, dst) in enumerate(((xg, 7, 8), (xc, 7, 8), (xk, 0, 1)))
        ]

    copy_a = remote(chg, ac, send_a, recv_a, down1)

    def slot_copies(src, slot, half, where):
        return [
            remote(
                ref.at[src, half], ref.at[slot, half], send_x.at[i, slot, half],
                recv_x.at[i, slot, half], where,
            )
            for i, ref in enumerate((xg, xc))
        ]

    def spread(src, half, upward):
        @pl.when(core == 1 - upward)
        def _():
            for copy in slot_copies(src, 0, half, partner):
                copy.start()

        for step in range(1, 4):

            @pl.when((chip + step < 4) == (upward == 1))
            def _():
                for copy in slot_copies(src, step, half, peer(step)):
                    copy.start()

    def partner_back(step, half):
        return remote(
            sp.at[step, half], pb.at[step, half], send_p.at[step, half], recv_p.at[step, half],
            partner,
        )

    def peer_back(step, half):
        return remote(
            sq.at[step, half], rb.at[step, half], send_b.at[step, half], recv_b.at[step, half],
            peer(4 - step),
        )

    def to_mate(half):
        return remote(sy.at[half], ry.at[half], send_m.at[half], recv_m.at[half], mate)

    def home(half):
        return remote(sh.at[half], rh.at[half], send_h.at[half], recv_h.at[half], near_src)

    for load in loads:
        load.wait()
    own = geo[...]
    feat[...] = jnp.concatenate(features(own)[0], axis=0).T.astype(BF16)
    wown[...] = (chg[...].astype(F32) * (own[3:4] * own[3:4])).astype(BF16)
    pot_ref[...] = jnp.zeros_like(pot_ref)

    def visit(other_geo, other_chg):
        right[...] = jnp.concatenate(features(other_geo)[1], axis=0).astype(BF16)
        woth[...] = (other_chg.astype(F32) * (other_geo[3:4] * other_geo[3:4])).astype(BF16)
        back[...] = jnp.zeros_like(back)
        tiles = (tile_a, tile_b)

        def fill(r):
            squared = jnp.dot(
                feat[r * ROWBLK : (r + 1) * ROWBLK, :], right[...], preferred_element_type=F32
            )
            tiles[r % 2][...] = lax.rsqrt(squared).astype(BF16)

        fill(0)
        for r in range(BLOCK // ROWBLK):
            if r + 1 < BLOCK // ROWBLK:
                fill(r + 1)
            rows = slice(r * ROWBLK, (r + 1) * ROWBLK)
            tile = tiles[r % 2][...]
            pot_ref[:, rows] += lax.dot_general(woth[...], tile, NT, preferred_element_type=F32)
            back[...] += jnp.dot(wown[:, rows], tile, preferred_element_type=F32)

    def own_half(half):
        lanes = pl.ds(pl.multiple_of(half * HALF, HALF), HALF)
        visit(geo[:, lanes], chg[:, lanes])

    own_half(0)
    pl.semaphore_wait(barrier, 30)
    for half in range(HALVES):
        for copy in w_copies(half):
            copy.start()
    copy_a.start()
    own_half(1)
    for half in range(HALVES):
        for copy in w_copies(half):
            copy.wait_recv()

        @pl.when(far)
        def _():
            for copy in y_copies(half):
                copy.start()

        spread(7, half, near_flag)

    def near_group(g, carry):
        index = ni[pl.ds(g, 1), :]
        lane = lax.broadcasted_iota(jnp.int32, (1, 128), 1)
        index = jnp.where(lane < nc_ref[g], index, -1)
        slot = lax.broadcasted_iota(jnp.int32, (HALF, 128), 0)
        taken = jnp.zeros((RHS, 128), F32)
        sources = (
            xc[upper_slot, 0], xc[upper_slot, 1], chg[:, :HALF], chg[:, HALF:],
            ac[:, :HALF], ac[:, HALF:],
        )
        for part, source in enumerate(sources):
            pick = jnp.where(slot == index - part * HALF, 1.0, 0.0).astype(BF16)
            taken = taken + jnp.dot(source, pick, preferred_element_type=F32)
        columns = pl.ds(pl.multiple_of(g * 128, 128), 128)
        pot_ref[:, columns] += lax.dot_general(
            taken.astype(BF16), nw[g], NT, preferred_element_type=F32
        )
        return carry

    def near_field():
        copy_a.wait_recv()
        lax.fori_loop(0, GROUPS, near_group, 0)

    pl.when(near_field_early)(near_field)

    def slot_of(t):
        rest = t - 2 * early
        is_late = rest >= 0
        second = rest >= late
        index = jnp.where(is_late, early + rest - jnp.where(second, late, 0), t // 2)
        half = jnp.where(is_late, second.astype(jnp.int32), lax.rem(t, 2))
        index = index - near_flag
        k = index - lead
        dist = jnp.where(near_up, k // 2 + 1, 3 - k // 2)
        slot = jnp.where((k < 0) | (k == 6), 0, dist + 3 * lax.rem(k + 2, 2))
        return jnp.where((index < 0) | (index == 7), upper_slot, slot), half

    def late_gather(t):
        slot, half = slot_of(jnp.maximum(t, 0))

        @pl.when((t >= 0) & (slot >= 1) & (slot <= 3))
        def _():
            partner_back(slot, half).wait_recv()
            sq[slot, half] = (keep[slot, half] + pb[slot, half].astype(F32)).astype(BF16)
            peer_back(slot, half).start()

    def step_(t, carry):
        for half, at in ((0, jnp.minimum(SEND_FIRST, 2 * early)),
                         (1, jnp.minimum(SEND_SECOND, 2 * early + late))):

            @pl.when((t == at) & far)
            def _():
                for copy in y_copies(half):
                    copy.wait_recv()
                spread(8, half, 1 - near_flag)

        slot, half = slot_of(t)
        direct = (slot >= 1) & (slot <= 3)

        @pl.when(slot < 7)
        def _():
            for copy in slot_copies(7, slot, half, partner):
                copy.wait_recv()

        @pl.when(direct)
        def _():
            for copy in slot_copies(slot, slot + 3, half, partner):
                copy.start()

        visit(xg[slot, half], xc[slot, half])

        @pl.when(direct)
        def _():
            keep[slot, half] = back[...]

        @pl.when(slot >= 7)
        def _():
            keep[0, half] = back[...]

        @pl.when((slot == 0) | ((slot >= 4) & (slot <= 6)))
        def _():
            step = jnp.where(slot == 0, 0, slot - 3)
            sp[step, half] = back[...].astype(BF16)
            partner_back(step, half).start()

        late_gather(t - 4)
        return carry

    lax.fori_loop(0, 16, step_, 0)

    def tail(t, carry):
        late_gather(t)
        return carry

    lax.fori_loop(12, 16, tail, 0)
    total[...] = jnp.zeros_like(total)

    def collect(dst, half, upward):
        dst[half] = keep[0, half] * upward.astype(F32)

        @pl.when(core == 1 - upward)
        def _():
            partner_back(0, half).wait_recv()
            dst[half] += pb[0, half].astype(F32)

        for step in range(1, 4):

            @pl.when((chip + step < 4) == (upward == 1))
            def _():
                peer_back(step, half).wait_recv()
                dst[half] += rb[step, half].astype(F32)

    @pl.when(far)
    def _():
        def one(half, carry):
            collect(acc_w, half, 1 - near_flag)
            sy[half] = acc_w[half].astype(BF16)
            to_mate(half).start()
            return carry

        lax.fori_loop(0, HALVES, one, 0)

        def more(half, carry):
            total[...] += member_totals(acc_w[half], xg[8, half][3:4], xk[1, half])
            return carry

        lax.fori_loop(0, HALVES, more, 0)

    def near_sum(half, carry):
        collect(acc_w, half, near_flag)
        total[...] += member_totals(acc_w[half], xg[7, half][3:4], xk[0, half])
        return carry

    lax.fori_loop(0, HALVES, near_sum, 0)
    pl.when(jnp.logical_not(near_field_early))(near_field)
    total[...] += member_totals(pot_ref[...], own[3:4], cond[...])

    local = total[...]
    value = jnp.concatenate([local[q * 8 : q * 8 + 8] for q in range(4)], axis=1)
    sent = 0
    total_copies = []
    for count, mine, where, slots, recv in (
        (8, place, in_group, s1, recv1),
        (4, yplace, in_y, s2, recv2),
        (16, zplace, in_z, s3, recv3),
    ):
        slots[mine] = value
        stage = []
        for step in range(1, count):
            stage.append(
                remote(slots.at[mine], slots.at[mine], send_t.at[sent], recv.at[step], where(step))
            )
            sent += 1
        for copy in stage:
            copy.start()
        if count == 16:
            for half in range(HALVES):

                @pl.when(far)
                def _():
                    to_mate(half).wait_recv()
                    acc_w[half] += ry[half].astype(F32)

                sh[half] = acc_w[half].astype(BF16)
                home(half).start()
        for copy in stage:
            copy.wait_recv()
        value = slots[0]
        for other in range(1, count):
            value = value + slots[other]
        total_copies += stage
    tot_ref[...] = value

    for half in range(HALVES):
        lanes = slice(half * HALF, (half + 1) * HALF)
        home(half).wait_recv()
        pot_ref[:, lanes] += rh[half].astype(F32)

    copy_a.wait_send()
    for copy in total_copies:
        copy.wait_send()

    def drain(half, carry):
        for copy in w_copies(half):
            copy.wait_send()
        home(half).wait_send()

        @pl.when(far)
        def _():
            for copy in y_copies(half):
                copy.wait_send()
            to_mate(half).wait_send()

        for slot in range(7):
            for copy in slot_copies(7, slot, half, partner):
                copy.wait_send()
        for step in range(4):
            partner_back(step, half).wait_send()
        for step in range(1, 4):
            peer_back(step, half).wait_send()
        return carry

    lax.fori_loop(0, HALVES, drain, 0)


def on_device(geometry, charges, near_index, near_count, near_weight, conductor):
    def half(kind, *lead, rows=RHS):
        return pltpu.VMEM((*lead, HALVES, rows, HALF), kind)

    dma = pltpu.SemaphoreType.DMA
    potential, packed = pl.pallas_call(
        kernel,
        out_shape=(
            jax.ShapeDtypeStruct((RHS, BLOCK), F32),
            jax.ShapeDtypeStruct((8, 128), F32),
        ),
        in_specs=[HBM, HBM, HBM, SMEM, HBM, HBM],
        out_specs=(VMEM, VMEM),
        scratch_shapes=[
            pltpu.VMEM((4, BLOCK), F32), pltpu.VMEM((RHS, BLOCK), BF16),
            pltpu.VMEM((GROUPS, 128), jnp.int32), pltpu.VMEM((GROUPS, 128, 128), BF16),
            pltpu.VMEM((1, BLOCK), jnp.int32), dma((5,)),
            pltpu.VMEM((BLOCK, 40), BF16), pltpu.VMEM((40, HALF), BF16),
            pltpu.VMEM((RHS, BLOCK), BF16), pltpu.VMEM((RHS, HALF), BF16),
            pltpu.VMEM((RHS, HALF), F32), half(F32), half(F32, 4), pltpu.VMEM((RHS, RHS), F32),
            pltpu.VMEM((ROWBLK, HALF), BF16), pltpu.VMEM((ROWBLK, HALF), BF16),
            half(F32, 9, rows=4), half(BF16, 9), half(jnp.int32, 2, rows=1),
            pltpu.VMEM((RHS, BLOCK), BF16), half(BF16, 4), half(BF16, 4), half(BF16, 4),
            half(BF16, 4), half(BF16), half(BF16), half(BF16), half(BF16),
            pltpu.VMEM((8, 8, 128), F32), pltpu.VMEM((4, 8, 128), F32),
            pltpu.VMEM((16, 8, 128), F32),
            dma((3, 2)), dma((3, 2)), dma((3, 2)), dma((3, 2)), dma, dma,
            dma((2, 7, 2)), dma((2, 7, 2)), dma((4, 2)), dma((4, 2)), dma((4, 2)), dma((4, 2)),
            dma((2,)), dma((2,)), dma((2,)), dma((2,)), dma((25,)), dma((8,)), dma((4,)),
            dma((16,)),
        ],
        compiler_params=pltpu.CompilerParams(
            collective_id=0, has_side_effects=True, vmem_limit_bytes=48 * 2**20
        ),
        name="potential",
    )(geometry, charges, near_index, near_count, near_weight, conductor.reshape(1, BLOCK))
    totals = packed.reshape(8, 4, RHS).transpose(1, 0, 2).reshape(RHS, RHS)
    return potential, totals


def solution(mesh):
    in_specs = (
        P(None, ("row", "col")),
        P(None, ("row", "col")),
        P(("row", "col"), None),
        P(("row", "col")),
        P(("row", "col"), None, None),
        P(("row", "col")),
    )
    out_specs = (P(None, ("row", "col")), P())
    return jax.shard_map(
        on_device, mesh=mesh, in_specs=in_specs, out_specs=out_specs, check_vma=False
    )
```

```python
import jax
import jax.numpy as jnp
from jax import lax
from jax.experimental import pallas as pl
from jax.experimental.pallas import tpu as pltpu
from jax.sharding import PartitionSpec as P

MESH = pl.DeviceIdType.MESH
BLOCK = 1536
CHUNKS = 2
WIDTH = BLOCK // CHUNKS
RHS = 32
GROUPS = 12
ROWBLK = 256
ROWS = 16
COLS = 32
STEPS = 8 * CHUNKS
PASS_ON = (4, 7)
VMEM_BYTES = 62 * 2**20
F32 = jnp.float32
BF16 = jnp.bfloat16
VMEM = pl.BlockSpec(memory_space=pltpu.VMEM)
SMEM = pl.BlockSpec(memory_space=pltpu.SMEM)
HBM = pl.BlockSpec(memory_space=pltpu.HBM)
NT = (((1,), (1,)), ((), ()))


def three(v):
    high = v.astype(BF16).astype(F32)
    rest = v - high
    mid = rest.astype(BF16).astype(F32)
    return high, mid, rest - mid


def features(geo):
    high, mid, low = three(geo[0:3])
    norm = (
        geo[0:1] * geo[0:1] + geo[1:2] * geo[1:2] + geo[2:3] * geo[2:3] + geo[3:4] * geo[3:4]
    )
    nh, nm, nl = three(norm)
    one = jnp.ones_like(norm)
    pad = jnp.zeros((7, geo.shape[1]), F32)
    left = [high, high, high, mid, mid, mid, low, low, low, nh, nm, nl, one, one, one, pad]
    h2, m2, l2 = -2.0 * high, -2.0 * mid, -2.0 * low
    right = [h2, m2, l2, h2, m2, l2, h2, m2, l2, one, one, one, nh, nm, nl, pad]
    return left, right


def shifted(row, col, steps):
    flat = lax.rem(row * COLS + col + (steps + 2 * ROWS * COLS), ROWS * COLS)
    return flat // COLS, lax.rem(flat, COLS)


def member_totals(value, size, conductor):
    pieces = three(value * (size * size))
    slot = lax.broadcasted_iota(jnp.int32, (RHS, value.shape[1]), 0)
    member = jnp.where(slot == conductor, 1.0, 0.0).astype(BF16)
    total = jnp.zeros((RHS, RHS), F32)
    for piece in pieces:
        total = total + lax.dot_general(
            piece.astype(BF16), member, NT, preferred_element_type=F32
        )
    return total


def kernel(
    geo_in, chg_in, ni_in, nc_ref, nw_in, cond_in, pot_ref, tot_ref,
    geo, chg, ni, nw, cond, in_sem,
    feat, right, wown, woth, back, acc_w, keep, total, tile_a, tile_b, flip_a, flip_b,
    xg, xc, xk, ac, sp, sq, pb, rb, sy, ry, sh, rh, s1, s2, s3,
    send_w, recv_w, send_y, recv_y, send_a, recv_a, send_x, recv_x, send_p, recv_p,
    send_b, recv_b, send_m, recv_m, send_h, recv_h, send_t, recv1, recv2, recv3,
):
    row = lax.axis_index("row")
    col = lax.axis_index("col")
    zhigh = row // 8
    place = lax.rem(row, 8)
    chip = place // 2
    core = lax.rem(place, 2)
    yplace = col // 8
    zlow = lax.rem(col, 8)
    zplace = zhigh * 8 + zlow
    up1 = shifted(row, col, 1)
    down1 = shifted(row, col, -1)
    near_dst = shifted(row, col, jnp.where(zlow == 7, 257, 1))
    near_src = shifted(row, col, jnp.where(zlow == 0, -257, -1))
    mate = (lax.rem(row + 8, ROWS), col)
    partner = (zhigh * 8 + chip * 2 + 1 - core, col)
    near_up = zlow != 0
    near_flag = near_up.astype(jnp.int32)
    far = jnp.logical_not(near_up & (place == 0))
    upper_slot = 8 - near_flag
    early = jnp.where(near_up, place + 1, 7 - place)
    late = 8 - early
    lead = jnp.where(near_up, core, 1 - core)
    near_field_early = near_up & (zlow != 7)

    def peer(step):
        return zhigh * 8 + lax.rem(chip + step, 4) * 2 + core, col

    def in_group(step):
        return zhigh * 8 + lax.rem(place + step, 8), col

    def in_y(step):
        return row, lax.rem(yplace + step, 4) * 8 + zlow

    def in_z(step):
        other = lax.rem(zplace + step, 16)
        return (other // 8) * 8 + place, yplace * 8 + lax.rem(other, 8)

    barrier = pltpu.get_barrier_semaphore()
    for other in (mate, near_dst, near_src, up1, down1):
        pl.semaphore_signal(barrier, inc=1, device_id=other, device_id_type=MESH)
    for count, where in ((16, in_z), (4, in_y), (8, in_group)):
        for step in range(1, count):
            pl.semaphore_signal(barrier, inc=1, device_id=where(step), device_id_type=MESH)

    loads = [
        pltpu.make_async_copy(src, dst, in_sem.at[i])
        for i, (src, dst) in enumerate(
            ((geo_in, geo), (chg_in, chg), (ni_in, ni), (nw_in, nw), (cond_in, cond))
        )
    ]
    for load in loads:
        load.start()

    def remote(src, dst, ssem, rsem, where):
        return pltpu.make_async_remote_copy(
            src_ref=src, dst_ref=dst, send_sem=ssem, recv_sem=rsem, device_id=where,
            device_id_type=MESH,
        )

    def w_copies(half):
        lanes = pl.ds(half * WIDTH, WIDTH)
        return [
            remote(
                src.at[:, lanes], dst.at[half], send_w.at[i, half], recv_w.at[i, half], near_dst
            )
            for i, (src, dst) in enumerate(
                zip((geo, chg, cond), (xg.at[7], xc.at[7], xk.at[0]))
            )
        ]

    def y_copies(half):
        return [
            remote(
                ref.at[src, half], ref.at[dst, half], send_y.at[i, half], recv_y.at[i, half], mate
            )
            for i, (ref, src, dst) in enumerate(((xg, 7, 8), (xc, 7, 8), (xk, 0, 1)))
        ]

    copy_a = remote(chg, ac, send_a, recv_a, down1)

    def slot_copies(src, slot, half, where):
        return [
            remote(
                ref.at[src, half], ref.at[slot, half], send_x.at[i, slot, half],
                recv_x.at[i, slot, half], where,
            )
            for i, ref in enumerate((xg, xc))
        ]

    def spread(src, half, upward):
        @pl.when(core == 1 - upward)
        def _():
            for copy in slot_copies(src, 0, half, partner):
                copy.start()

        for step in range(1, 4):

            @pl.when((chip + step < 4) == (upward == 1))
            def _():
                for copy in slot_copies(src, step, half, peer(step)):
                    copy.start()

    def partner_back(step, half):
        return remote(
            sp.at[step, half], pb.at[step, half], send_p.at[step, half], recv_p.at[step, half],
            partner,
        )

    def peer_back(step, half):
        return remote(
            sq.at[step, half], rb.at[step, half], send_b.at[step, half], recv_b.at[step, half],
            peer(4 - step),
        )

    def to_mate(half):
        return remote(sy.at[half], ry.at[half], send_m.at[half], recv_m.at[half], mate)

    def home(half):
        return remote(sh.at[half], rh.at[half], send_h.at[half], recv_h.at[half], near_src)

    for load in loads:
        load.wait()
    own = geo[...]
    feat[...] = jnp.concatenate(features(own)[0], axis=0).T.astype(BF16)
    wown[...] = (chg[...].astype(F32) * (own[3:4] * own[3:4])).astype(BF16)
    pot_ref[...] = jnp.zeros_like(pot_ref)

    def visit(other_geo, other_chg):
        right[...] = jnp.concatenate(features(other_geo)[1], axis=0).astype(BF16)
        woth[...] = (other_chg.astype(F32) * (other_geo[3:4] * other_geo[3:4])).astype(BF16)
        back[...] = jnp.zeros_like(back)
        tiles, flips = (tile_a, tile_b), (flip_a, flip_b)

        def fill(r):
            squared = jnp.dot(
                feat[r * ROWBLK : (r + 1) * ROWBLK, :], right[...], preferred_element_type=F32
            )
            tile = lax.rsqrt(squared).astype(BF16)
            tiles[r % 2][...] = tile
            flips[r % 2][...] = tile.T

        fill(0)
        for r in range(BLOCK // ROWBLK):
            if r + 1 < BLOCK // ROWBLK:
                fill(r + 1)
            rows = slice(r * ROWBLK, (r + 1) * ROWBLK)
            pot_ref[:, rows] += jnp.dot(woth[...], flips[r % 2][...], preferred_element_type=F32)
            back[...] += jnp.dot(wown[:, rows], tiles[r % 2][...], preferred_element_type=F32)

    def own_half(half):
        lanes = pl.ds(pl.multiple_of(half * WIDTH, WIDTH), WIDTH)
        visit(geo[:, lanes], chg[:, lanes])

    own_half(0)
    pl.semaphore_wait(barrier, 30)
    for half in range(CHUNKS):
        for copy in w_copies(half):
            copy.start()
    copy_a.start()
    for half in range(CHUNKS):
        if half + 1 < CHUNKS:
            own_half(half + 1)
        for copy in w_copies(half):
            copy.wait_recv()

        @pl.when(far)
        def _():
            for copy in y_copies(half):
                copy.start()

        spread(7, half, near_flag)

    def near_group(g, carry):
        index = ni[pl.ds(g, 1), :]
        lane = lax.broadcasted_iota(jnp.int32, (1, 128), 1)
        index = jnp.where(lane < nc_ref[g], index, -1)
        slot = lax.broadcasted_iota(jnp.int32, (WIDTH, 128), 0)
        taken = jnp.zeros((RHS, 128), F32)
        sources = [xc[upper_slot, c] for c in range(CHUNKS)]
        for ref in (chg, ac):
            sources += [ref[:, c * WIDTH : (c + 1) * WIDTH] for c in range(CHUNKS)]
        for part, source in enumerate(sources):
            pick = jnp.where(slot == index - part * WIDTH, 1.0, 0.0).astype(BF16)
            taken = taken + jnp.dot(source, pick, preferred_element_type=F32)
        columns = pl.ds(pl.multiple_of(g * 128, 128), 128)
        pot_ref[:, columns] += lax.dot_general(
            taken.astype(BF16), nw[g], NT, preferred_element_type=F32
        )
        return carry

    def near_field():
        copy_a.wait_recv()
        lax.fori_loop(0, GROUPS, near_group, 0)

    pl.when(near_field_early)(near_field)

    def slot_of(t):
        rest = t - CHUNKS * early
        is_late = rest >= 0
        turn = sum((rest >= c * late).astype(jnp.int32) for c in range(1, CHUNKS))
        index = jnp.where(is_late, early + rest - turn * late, t // CHUNKS)
        half = jnp.where(is_late, turn, lax.rem(t, CHUNKS))
        index = index - near_flag
        k = index - lead
        dist = jnp.where(near_up, k // 2 + 1, 3 - k // 2)
        slot = jnp.where((k < 0) | (k == 6), 0, dist + 3 * lax.rem(k + 2, 2))
        return jnp.where((index < 0) | (index == 7), upper_slot, slot), half

    def gather(t, wanted):
        slot, half = slot_of(jnp.maximum(t, 0))

        @pl.when(wanted & (t >= 0) & (slot >= 1) & (slot <= 3))
        def _():
            partner_back(slot, half).wait_recv()
            sq[slot, half] = (keep[slot, half] + pb[slot, half].astype(F32)).astype(BF16)
            peer_back(slot, half).start()

    def is_early(t):
        return t < CHUNKS * early

    def step_(t, carry):
        for half in range(CHUNKS):
            at = jnp.minimum(PASS_ON[half], CHUNKS * early + half * late)

            @pl.when((t == at) & far)
            def _():
                for copy in y_copies(half):
                    copy.wait_recv()
                spread(8, half, 1 - near_flag)

        slot, half = slot_of(t)
        direct = (slot >= 1) & (slot <= 3)

        @pl.when(slot < 7)
        def _():
            for copy in slot_copies(7, slot, half, partner):
                copy.wait_recv()

        @pl.when(direct)
        def _():
            for copy in slot_copies(slot, slot + 3, half, partner):
                copy.start()

        visit(xg[slot, half], xc[slot, half])

        @pl.when(direct)
        def _():
            keep[slot, half] = back[...]

        @pl.when(slot >= 7)
        def _():
            keep[0, half] = back[...]

        @pl.when((slot == 0) | ((slot >= 4) & (slot <= 6)))
        def _():
            step = jnp.where(slot == 0, 0, slot - 3)
            sp[step, half] = back[...].astype(BF16)
            partner_back(step, half).start()

        gather(t - 2 * CHUNKS, is_early(t - 2 * CHUNKS))
        gather(t - 4, jnp.logical_not(is_early(t - 4)))
        return carry

    lax.fori_loop(0, STEPS, step_, 0)

    def tail(t, carry):
        gather(t, is_early(t) | (t >= STEPS - 4))
        return carry

    lax.fori_loop(STEPS - 2 * CHUNKS, STEPS, tail, 0)
    total[...] = jnp.zeros_like(total)

    def collect(dst, half, upward):
        dst[half] = keep[0, half] * upward.astype(F32)

        @pl.when(core == 1 - upward)
        def _():
            partner_back(0, half).wait_recv()
            dst[half] += pb[0, half].astype(F32)

        for step in range(1, 4):

            @pl.when((chip + step < 4) == (upward == 1))
            def _():
                peer_back(step, half).wait_recv()
                dst[half] += rb[step, half].astype(F32)

    @pl.when(far)
    def _():
        def one(half, carry):
            collect(acc_w, half, 1 - near_flag)
            sy[half] = acc_w[half].astype(BF16)
            to_mate(half).start()
            return carry

        lax.fori_loop(0, CHUNKS, one, 0)

        def more(half, carry):
            total[...] += member_totals(acc_w[half], xg[8, half][3:4], xk[1, half])
            return carry

        lax.fori_loop(0, CHUNKS, more, 0)

    def near_sum(half, carry):
        collect(acc_w, half, near_flag)
        total[...] += member_totals(acc_w[half], xg[7, half][3:4], xk[0, half])
        return carry

    lax.fori_loop(0, CHUNKS, near_sum, 0)
    pl.when(jnp.logical_not(near_field_early))(near_field)
    total[...] += member_totals(pot_ref[...], own[3:4], cond[...])

    local = total[...]
    value = jnp.concatenate([local[q * 8 : q * 8 + 8] for q in range(4)], axis=1)
    sent = 0
    total_copies = []
    for count, mine, where, slots, recv in (
        (8, place, in_group, s1, recv1),
        (4, yplace, in_y, s2, recv2),
        (16, zplace, in_z, s3, recv3),
    ):
        slots[mine] = value
        stage = []
        for step in range(1, count):
            stage.append(
                remote(slots.at[mine], slots.at[mine], send_t.at[sent], recv.at[step], where(step))
            )
            sent += 1
        for copy in stage:
            copy.start()
        if count == 16:
            for half in range(CHUNKS):

                @pl.when(far)
                def _():
                    to_mate(half).wait_recv()
                    acc_w[half] += ry[half].astype(F32)

                sh[half] = acc_w[half].astype(BF16)
                home(half).start()
        for copy in stage:
            copy.wait_recv()
        value = slots[0]
        for other in range(1, count):
            value = value + slots[other]
        total_copies += stage
    for q in range(4):
        tot_ref[q * 8 : q * 8 + 8, :] = value[:, q * RHS : (q + 1) * RHS]

    for half in range(CHUNKS):
        lanes = slice(half * WIDTH, (half + 1) * WIDTH)
        home(half).wait_recv()
        pot_ref[:, lanes] += rh[half].astype(F32)

    copy_a.wait_send()
    for copy in total_copies:
        copy.wait_send()

    def drain(half, carry):
        for copy in w_copies(half):
            copy.wait_send()
        home(half).wait_send()

        @pl.when(far)
        def _():
            for copy in y_copies(half):
                copy.wait_send()
            to_mate(half).wait_send()

        for slot in range(7):
            for copy in slot_copies(7, slot, half, partner):
                copy.wait_send()
        for step in range(4):
            partner_back(step, half).wait_send()
        for step in range(1, 4):
            peer_back(step, half).wait_send()
        return carry

    lax.fori_loop(0, CHUNKS, drain, 0)


def on_device(geometry, charges, near_index, near_count, near_weight, conductor):
    def half(kind, *lead, rows=RHS):
        return pltpu.VMEM((*lead, CHUNKS, rows, WIDTH), kind)

    dma = pltpu.SemaphoreType.DMA
    potential, totals = pl.pallas_call(
        kernel,
        out_shape=(
            jax.ShapeDtypeStruct((RHS, BLOCK), F32),
            jax.ShapeDtypeStruct((RHS, RHS), F32),
        ),
        in_specs=[HBM, HBM, HBM, SMEM, HBM, HBM],
        out_specs=(VMEM, VMEM),
        scratch_shapes=[
            pltpu.VMEM((4, BLOCK), F32), pltpu.VMEM((RHS, BLOCK), BF16),
            pltpu.VMEM((GROUPS, 128), jnp.int32), pltpu.VMEM((GROUPS, 128, 128), BF16),
            pltpu.VMEM((1, BLOCK), jnp.int32), dma((5,)),
            pltpu.VMEM((BLOCK, 40), BF16), pltpu.VMEM((40, WIDTH), BF16),
            pltpu.VMEM((RHS, BLOCK), BF16), pltpu.VMEM((RHS, WIDTH), BF16),
            pltpu.VMEM((RHS, WIDTH), F32), half(F32), half(F32, 4), pltpu.VMEM((RHS, RHS), F32),
            *[pltpu.VMEM((ROWBLK, WIDTH), BF16)] * 2, *[pltpu.VMEM((WIDTH, ROWBLK), BF16)] * 2,
            half(F32, 9, rows=4), half(BF16, 9), half(jnp.int32, 2, rows=1),
            pltpu.VMEM((RHS, BLOCK), BF16), half(BF16, 4), half(BF16, 4), half(BF16, 4),
            half(BF16, 4), half(BF16), half(BF16), half(BF16), half(BF16),
            pltpu.VMEM((8, 8, 128), F32), pltpu.VMEM((4, 8, 128), F32),
            pltpu.VMEM((16, 8, 128), F32),
            *[dma((3, CHUNKS))] * 4, dma, dma, *[dma((2, 7, CHUNKS))] * 2,
            *[dma((4, CHUNKS))] * 4, *[dma((CHUNKS,))] * 4, dma((25,)), dma((8,)), dma((4,)),
            dma((16,)),
        ],
        compiler_params=pltpu.CompilerParams(
            collective_id=0, has_side_effects=True, vmem_limit_bytes=VMEM_BYTES
        ),
        name="potential",
    )(geometry, charges, near_index, near_count, near_weight, conductor.reshape(1, BLOCK))
    return potential, totals


def solution(mesh):
    in_specs = (
        P(None, ("row", "col")),
        P(None, ("row", "col")),
        P(("row", "col"), None),
        P(("row", "col")),
        P(("row", "col"), None, None),
        P(("row", "col")),
    )
    out_specs = (P(None, ("row", "col")), P())
    return jax.shard_map(
        on_device, mesh=mesh, in_specs=in_specs, out_specs=out_specs, check_vma=False
    )
```

```python
import jax
import jax.numpy as jnp
from jax import lax
from jax.experimental import pallas as pl
from jax.experimental.pallas import tpu as pltpu
from jax.sharding import PartitionSpec as P

MESH = pl.DeviceIdType.MESH
BLOCK = 1536
CHUNKS = 2
WIDTH = BLOCK // CHUNKS
RHS = 32
GROUPS = 12
ROWBLK = 384
ROWS = 16
COLS = 32
STEPS = 8 * CHUNKS
PASS_ON = (4, 7)
FIRST_HOME = 4
VMEM_BYTES = 62 * 2**20
F32 = jnp.float32
BF16 = jnp.bfloat16
VMEM = pl.BlockSpec(memory_space=pltpu.VMEM)
SMEM = pl.BlockSpec(memory_space=pltpu.SMEM)
HBM = pl.BlockSpec(memory_space=pltpu.HBM)
NT = (((1,), (1,)), ((), ()))


def three(v):
    high = v.astype(BF16).astype(F32)
    rest = v - high
    mid = rest.astype(BF16).astype(F32)
    return high, mid, rest - mid


def features(geo):
    high, mid, low = three(geo[0:3])
    norm = (
        geo[0:1] * geo[0:1] + geo[1:2] * geo[1:2] + geo[2:3] * geo[2:3] + geo[3:4] * geo[3:4]
    )
    nh, nm, nl = three(norm)
    one = jnp.ones_like(norm)
    pad = jnp.zeros((7, geo.shape[1]), F32)
    left = [high, high, high, mid, mid, mid, low, low, low, nh, nm, nl, one, one, one, pad]
    h2, m2, l2 = -2.0 * high, -2.0 * mid, -2.0 * low
    right = [h2, m2, l2, h2, m2, l2, h2, m2, l2, one, one, one, nh, nm, nl, pad]
    return left, right


def shifted(row, col, steps):
    flat = lax.rem(row * COLS + col + (steps + 2 * ROWS * COLS), ROWS * COLS)
    return flat // COLS, lax.rem(flat, COLS)


def member_totals(value, size, conductor):
    pieces = three(value * (size * size))
    slot = lax.broadcasted_iota(jnp.int32, (RHS, value.shape[1]), 0)
    member = jnp.where(slot == conductor, 1.0, 0.0).astype(BF16)
    total = jnp.zeros((RHS, RHS), F32)
    for piece in pieces:
        total = total + lax.dot_general(
            piece.astype(BF16), member, NT, preferred_element_type=F32
        )
    return total


def kernel(
    geo_in, chg_in, ni_in, nc_ref, nw_in, cond_in, pot_ref, tot_ref,
    geo, chg, ni, nw, cond, in_sem,
    feat, right, wown, woth, back, acc_w, keep, total, tile_a, tile_b, flip_a, flip_b,
    xg, xc, xk, ac, sp, sq, pb, rb, sy, ry, sh, rh, s1, s2, s3,
    send_w, recv_w, send_y, recv_y, send_a, recv_a, send_x, recv_x, send_p, recv_p,
    send_b, recv_b, send_m, recv_m, send_h, recv_h, send_t, recv1, recv2, recv3,
):
    row = lax.axis_index("row")
    col = lax.axis_index("col")
    zhigh = row // 8
    place = lax.rem(row, 8)
    chip = place // 2
    core = lax.rem(place, 2)
    yplace = col // 8
    zlow = lax.rem(col, 8)
    zplace = zhigh * 8 + zlow
    up1 = shifted(row, col, 1)
    down1 = shifted(row, col, -1)
    near_dst = shifted(row, col, jnp.where(zlow == 7, 257, 1))
    near_src = shifted(row, col, jnp.where(zlow == 0, -257, -1))
    mate = (lax.rem(row + 8, ROWS), col)
    partner = (zhigh * 8 + chip * 2 + 1 - core, col)
    near_up = zlow != 0
    near_flag = near_up.astype(jnp.int32)
    far = jnp.logical_not(near_up & (place == 0))
    upper_slot = 8 - near_flag
    early = jnp.where(near_up, place + 1, 7 - place)
    late = 8 - early
    lead = jnp.where(near_up, core, 1 - core)
    near_field_early = near_up & (zlow != 7)

    def peer(step):
        return zhigh * 8 + lax.rem(chip + step, 4) * 2 + core, col

    def in_group(step):
        return zhigh * 8 + lax.rem(place + step, 8), col

    def in_y(step):
        return row, lax.rem(yplace + step, 4) * 8 + zlow

    def in_z(step):
        other = lax.rem(zplace + step, 16)
        return (other // 8) * 8 + place, yplace * 8 + lax.rem(other, 8)

    barrier = pltpu.get_barrier_semaphore()
    for other in (mate, near_dst, near_src, up1, down1):
        pl.semaphore_signal(barrier, inc=1, device_id=other, device_id_type=MESH)
    for count, where in ((16, in_z), (4, in_y), (8, in_group)):
        for step in range(1, count):
            pl.semaphore_signal(barrier, inc=1, device_id=where(step), device_id_type=MESH)

    loads = [
        pltpu.make_async_copy(src, dst, in_sem.at[i])
        for i, (src, dst) in enumerate(
            ((geo_in, geo), (chg_in, chg), (ni_in, ni), (nw_in, nw), (cond_in, cond))
        )
    ]
    for load in loads:
        load.start()

    def remote(src, dst, ssem, rsem, where):
        return pltpu.make_async_remote_copy(
            src_ref=src, dst_ref=dst, send_sem=ssem, recv_sem=rsem, device_id=where,
            device_id_type=MESH,
        )

    def w_copies(half):
        lanes = pl.ds(half * WIDTH, WIDTH)
        return [
            remote(
                src.at[:, lanes], dst.at[half], send_w.at[i, half], recv_w.at[i, half], near_dst
            )
            for i, (src, dst) in enumerate(
                zip((geo, chg, cond), (xg.at[7], xc.at[7], xk.at[0]))
            )
        ]

    def y_copies(half):
        return [
            remote(
                ref.at[src, half], ref.at[dst, half], send_y.at[i, half], recv_y.at[i, half], mate
            )
            for i, (ref, src, dst) in enumerate(((xg, 7, 8), (xc, 7, 8), (xk, 0, 1)))
        ]

    copy_a = remote(chg, ac, send_a, recv_a, down1)

    def slot_copies(src, slot, half, where):
        return [
            remote(
                ref.at[src, half], ref.at[slot, half], send_x.at[i, slot, half],
                recv_x.at[i, slot, half], where,
            )
            for i, ref in enumerate((xg, xc))
        ]

    def spread(src, half, upward):
        @pl.when(core == 1 - upward)
        def _():
            for copy in slot_copies(src, 0, half, partner):
                copy.start()

        for step in range(1, 4):

            @pl.when((chip + step < 4) == (upward == 1))
            def _():
                for copy in slot_copies(src, step, half, peer(step)):
                    copy.start()

    def partner_back(step, half):
        return remote(
            sp.at[step, half], pb.at[step, half], send_p.at[step, half], recv_p.at[step, half],
            partner,
        )

    def peer_back(step, half):
        return remote(
            sq.at[step, half], rb.at[step, half], send_b.at[step, half], recv_b.at[step, half],
            peer(4 - step),
        )

    def to_mate(half):
        return remote(sy.at[half], ry.at[half], send_m.at[half], recv_m.at[half], mate)

    def home(half):
        return remote(sh.at[half], rh.at[half], send_h.at[half], recv_h.at[half], near_src)

    for load in loads:
        load.wait()
    own = geo[...]
    feat[...] = jnp.concatenate(features(own)[0], axis=0).T.astype(BF16)
    wown[...] = (chg[...].astype(F32) * (own[3:4] * own[3:4])).astype(BF16)
    pot_ref[...] = jnp.zeros_like(pot_ref)

    def visit(other_geo, other_chg):
        right[...] = jnp.concatenate(features(other_geo)[1], axis=0).astype(BF16)
        woth[...] = (other_chg.astype(F32) * (other_geo[3:4] * other_geo[3:4])).astype(BF16)
        back[...] = jnp.zeros_like(back)
        tiles, flips = (tile_a, tile_b), (flip_a, flip_b)

        def fill(r):
            squared = jnp.dot(
                feat[r * ROWBLK : (r + 1) * ROWBLK, :], right[...], preferred_element_type=F32
            )
            tile = lax.rsqrt(squared).astype(BF16)
            tiles[r % 2][...] = tile
            flips[r % 2][...] = tile.T

        fill(0)
        for r in range(BLOCK // ROWBLK):
            if r + 1 < BLOCK // ROWBLK:
                fill(r + 1)
            rows = slice(r * ROWBLK, (r + 1) * ROWBLK)
            pot_ref[:, rows] += jnp.dot(woth[...], flips[r % 2][...], preferred_element_type=F32)
            back[...] += jnp.dot(wown[:, rows], tiles[r % 2][...], preferred_element_type=F32)

    def own_half(half):
        lanes = pl.ds(pl.multiple_of(half * WIDTH, WIDTH), WIDTH)
        visit(geo[:, lanes], chg[:, lanes])

    own_half(0)
    pl.semaphore_wait(barrier, 30)
    for half in range(CHUNKS):
        for copy in w_copies(half):
            copy.start()
    copy_a.start()
    for half in range(CHUNKS):
        if half + 1 < CHUNKS:
            own_half(half + 1)
        for copy in w_copies(half):
            copy.wait_recv()

        @pl.when(far)
        def _():
            for copy in y_copies(half):
                copy.start()

        spread(7, half, near_flag)

    def near_group(g, carry):
        index = ni[pl.ds(g, 1), :]
        lane = lax.broadcasted_iota(jnp.int32, (1, 128), 1)
        index = jnp.where(lane < nc_ref[g], index, -1)
        slot = lax.broadcasted_iota(jnp.int32, (WIDTH, 128), 0)
        taken = jnp.zeros((RHS, 128), F32)
        sources = [xc[upper_slot, c] for c in range(CHUNKS)]
        for ref in (chg, ac):
            sources += [ref[:, c * WIDTH : (c + 1) * WIDTH] for c in range(CHUNKS)]
        for part, source in enumerate(sources):
            pick = jnp.where(slot == index - part * WIDTH, 1.0, 0.0).astype(BF16)
            taken = taken + jnp.dot(source, pick, preferred_element_type=F32)
        columns = pl.ds(pl.multiple_of(g * 128, 128), 128)
        pot_ref[:, columns] += lax.dot_general(
            taken.astype(BF16), nw[g], NT, preferred_element_type=F32
        )
        return carry

    def near_field():
        copy_a.wait_recv()
        lax.fori_loop(0, GROUPS, near_group, 0)

    pl.when(near_field_early)(near_field)

    def slot_of(t):
        rest = t - CHUNKS * early
        is_late = rest >= 0
        turn = sum((rest >= c * late).astype(jnp.int32) for c in range(1, CHUNKS))
        index = jnp.where(is_late, early + rest - turn * late, t // CHUNKS)
        half = jnp.where(is_late, turn, lax.rem(t, CHUNKS))
        index = index - near_flag
        k = index - lead
        dist = jnp.where(near_up, k // 2 + 1, 3 - k // 2)
        slot = jnp.where((k < 0) | (k == 6), 0, dist + 3 * lax.rem(k + 2, 2))
        return jnp.where((index < 0) | (index == 7), upper_slot, slot), half

    def gather(t, wanted):
        slot, half = slot_of(jnp.maximum(t, 0))

        @pl.when(wanted & (t >= 0) & (slot >= 1) & (slot <= 3))
        def _():
            partner_back(slot, half).wait_recv()
            sq[slot, half] = (keep[slot, half] + pb[slot, half].astype(F32)).astype(BF16)
            peer_back(slot, half).start()

    def is_early(t):
        return t < CHUNKS * early

    def collect(dst, half, upward):
        dst[half] = keep[0, half] * upward.astype(F32)

        @pl.when(core == 1 - upward)
        def _():
            partner_back(0, half).wait_recv()
            dst[half] += pb[0, half].astype(F32)

        for step in range(1, 4):

            @pl.when((chip + step < 4) == (upward == 1))
            def _():
                peer_back(step, half).wait_recv()
                dst[half] += rb[step, half].astype(F32)

    def far_sum(half):
        collect(acc_w, half, 1 - near_flag)
        sy[half] = acc_w[half].astype(BF16)
        to_mate(half).start()

    def step_(t, carry):
        for half in range(CHUNKS):
            at = jnp.minimum(PASS_ON[half], CHUNKS * early + half * late)

            @pl.when((t == at) & far)
            def _():
                for copy in y_copies(half):
                    copy.wait_recv()
                spread(8, half, 1 - near_flag)

        slot, half = slot_of(t)
        direct = (slot >= 1) & (slot <= 3)

        @pl.when(slot < 7)
        def _():
            for copy in slot_copies(7, slot, half, partner):
                copy.wait_recv()

        @pl.when(direct)
        def _():
            for copy in slot_copies(slot, slot + 3, half, partner):
                copy.start()

        visit(xg[slot, half], xc[slot, half])

        @pl.when(direct)
        def _():
            keep[slot, half] = back[...]

        @pl.when(slot >= 7)
        def _():
            keep[0, half] = back[...]

        @pl.when((slot == 0) | ((slot >= 4) & (slot <= 6)))
        def _():
            step = jnp.where(slot == 0, 0, slot - 3)
            sp[step, half] = back[...].astype(BF16)
            partner_back(step, half).start()

        @pl.when((t == jnp.minimum(CHUNKS * early + late + FIRST_HOME, STEPS - 1)) & far)
        def _():
            far_sum(0)

        gather(t - 2 * CHUNKS, is_early(t - 2 * CHUNKS))
        gather(t - 4, jnp.logical_not(is_early(t - 4)))
        return carry

    lax.fori_loop(0, STEPS, step_, 0)

    def tail(t, carry):
        gather(t, is_early(t) | (t >= STEPS - 4))
        return carry

    lax.fori_loop(STEPS - 2 * CHUNKS, STEPS, tail, 0)
    total[...] = jnp.zeros_like(total)

    @pl.when(far)
    def _():
        far_sum(1)

        def more(half, carry):
            total[...] += member_totals(acc_w[half], xg[8, half][3:4], xk[1, half])
            return carry

        lax.fori_loop(0, CHUNKS, more, 0)

    def near_sum(half, carry):
        collect(acc_w, half, near_flag)
        total[...] += member_totals(acc_w[half], xg[7, half][3:4], xk[0, half])
        return carry

    lax.fori_loop(0, CHUNKS, near_sum, 0)
    pl.when(jnp.logical_not(near_field_early))(near_field)
    total[...] += member_totals(pot_ref[...], own[3:4], cond[...])

    local = total[...]
    value = jnp.concatenate([local[q * 8 : q * 8 + 8] for q in range(4)], axis=1)
    sent = 0
    total_copies = []
    for count, mine, where, slots, recv in (
        (8, place, in_group, s1, recv1),
        (4, yplace, in_y, s2, recv2),
        (16, zplace, in_z, s3, recv3),
    ):
        slots[mine] = value
        stage = []
        for step in range(1, count):
            stage.append(
                remote(slots.at[mine], slots.at[mine], send_t.at[sent], recv.at[step], where(step))
            )
            sent += 1
        for copy in stage:
            copy.start()
        if count == 16:
            for half in range(CHUNKS):

                @pl.when(far)
                def _():
                    to_mate(half).wait_recv()
                    acc_w[half] += ry[half].astype(F32)

                sh[half] = acc_w[half].astype(BF16)
                home(half).start()
        for copy in stage:
            copy.wait_recv()
        value = slots[0]
        for other in range(1, count):
            value = value + slots[other]
        total_copies += stage
    for q in range(4):
        tot_ref[q * 8 : q * 8 + 8, :] = value[:, q * RHS : (q + 1) * RHS]

    for half in range(CHUNKS):
        lanes = slice(half * WIDTH, (half + 1) * WIDTH)
        home(half).wait_recv()
        pot_ref[:, lanes] += rh[half].astype(F32)

    copy_a.wait_send()
    for copy in total_copies:
        copy.wait_send()

    def drain(half, carry):
        for copy in w_copies(half):
            copy.wait_send()
        home(half).wait_send()

        @pl.when(far)
        def _():
            for copy in y_copies(half):
                copy.wait_send()
            to_mate(half).wait_send()

        for slot in range(7):
            for copy in slot_copies(7, slot, half, partner):
                copy.wait_send()
        for step in range(4):
            partner_back(step, half).wait_send()
        for step in range(1, 4):
            peer_back(step, half).wait_send()
        return carry

    lax.fori_loop(0, CHUNKS, drain, 0)


def on_device(geometry, charges, near_index, near_count, near_weight, conductor):
    def half(kind, *lead, rows=RHS):
        return pltpu.VMEM((*lead, CHUNKS, rows, WIDTH), kind)

    dma = pltpu.SemaphoreType.DMA
    potential, totals = pl.pallas_call(
        kernel,
        out_shape=(
            jax.ShapeDtypeStruct((RHS, BLOCK), F32),
            jax.ShapeDtypeStruct((RHS, RHS), F32),
        ),
        in_specs=[HBM, HBM, HBM, SMEM, HBM, HBM],
        out_specs=(VMEM, VMEM),
        scratch_shapes=[
            pltpu.VMEM((4, BLOCK), F32), pltpu.VMEM((RHS, BLOCK), BF16),
            pltpu.VMEM((GROUPS, 128), jnp.int32), pltpu.VMEM((GROUPS, 128, 128), BF16),
            pltpu.VMEM((1, BLOCK), jnp.int32), dma((5,)),
            pltpu.VMEM((BLOCK, 40), BF16), pltpu.VMEM((40, WIDTH), BF16),
            pltpu.VMEM((RHS, BLOCK), BF16), pltpu.VMEM((RHS, WIDTH), BF16),
            pltpu.VMEM((RHS, WIDTH), F32), half(F32), half(F32, 4), pltpu.VMEM((RHS, RHS), F32),
            *[pltpu.VMEM((ROWBLK, WIDTH), BF16)] * 2, *[pltpu.VMEM((WIDTH, ROWBLK), BF16)] * 2,
            half(F32, 9, rows=4), half(BF16, 9), half(jnp.int32, 2, rows=1),
            pltpu.VMEM((RHS, BLOCK), BF16), half(BF16, 4), half(BF16, 4), half(BF16, 4),
            half(BF16, 4), half(BF16), half(BF16), half(BF16), half(BF16),
            pltpu.VMEM((8, 8, 128), F32), pltpu.VMEM((4, 8, 128), F32),
            pltpu.VMEM((16, 8, 128), F32),
            *[dma((3, CHUNKS))] * 4, dma, dma, *[dma((2, 7, CHUNKS))] * 2,
            *[dma((4, CHUNKS))] * 4, *[dma((CHUNKS,))] * 4, dma((25,)), dma((8,)), dma((4,)),
            dma((16,)),
        ],
        compiler_params=pltpu.CompilerParams(
            collective_id=0, has_side_effects=True, vmem_limit_bytes=VMEM_BYTES
        ),
        name="potential",
    )(geometry, charges, near_index, near_count, near_weight, conductor.reshape(1, BLOCK))
    return potential, totals


def solution(mesh):
    in_specs = (
        P(None, ("row", "col")),
        P(None, ("row", "col")),
        P(("row", "col"), None),
        P(("row", "col")),
        P(("row", "col"), None, None),
        P(("row", "col")),
    )
    out_specs = (P(None, ("row", "col")), P())
    return jax.shard_map(
        on_device, mesh=mesh, in_specs=in_specs, out_specs=out_specs, check_vma=False
    )
```

```python
import jax
import jax.numpy as jnp
from jax import lax
from jax.experimental import pallas as pl
from jax.experimental.pallas import tpu as pltpu
from jax.sharding import PartitionSpec as P

MESH = pl.DeviceIdType.MESH
BLOCK = 1536
CHUNKS = 2
WIDTH = BLOCK // CHUNKS
RHS = 32
GROUPS = 12
ROWBLK = 384
ROWS = 16
COLS = 32
STEPS = 8 * CHUNKS
PASS_ON = (4, 7)
FIRST_HOME = 4
VMEM_BYTES = 62 * 2**20
F32 = jnp.float32
BF16 = jnp.bfloat16
VMEM = pl.BlockSpec(memory_space=pltpu.VMEM)
SMEM = pl.BlockSpec(memory_space=pltpu.SMEM)
HBM = pl.BlockSpec(memory_space=pltpu.HBM)
NT = (((1,), (1,)), ((), ()))


def three(v):
    high = v.astype(BF16).astype(F32)
    rest = v - high
    mid = rest.astype(BF16).astype(F32)
    return high, mid, rest - mid


def features(geo):
    high, mid, low = three(geo[0:3])
    norm = (
        geo[0:1] * geo[0:1] + geo[1:2] * geo[1:2] + geo[2:3] * geo[2:3] + geo[3:4] * geo[3:4]
    )
    nh, nm, nl = three(norm)
    one = jnp.ones_like(norm)
    pad = jnp.zeros((7, geo.shape[1]), F32)
    left = [high, high, high, mid, mid, mid, low, low, low, nh, nm, nl, one, one, one, pad]
    h2, m2, l2 = -2.0 * high, -2.0 * mid, -2.0 * low
    right = [h2, m2, l2, h2, m2, l2, h2, m2, l2, one, one, one, nh, nm, nl, pad]
    return left, right


def shifted(row, col, steps):
    flat = lax.rem(row * COLS + col + (steps + 2 * ROWS * COLS), ROWS * COLS)
    return flat // COLS, lax.rem(flat, COLS)


def member_totals(value, size, conductor):
    pieces = three(value * (size * size))
    slot = lax.broadcasted_iota(jnp.int32, (RHS, value.shape[1]), 0)
    member = jnp.where(slot == conductor, 1.0, 0.0).astype(BF16)
    total = jnp.zeros((RHS, RHS), F32)
    for piece in pieces:
        total = total + lax.dot_general(
            piece.astype(BF16), member, NT, preferred_element_type=F32
        )
    return total


def kernel(
    geo_in, chg_in, ni_in, nc_ref, nw_in, cond_in, pot_ref, tot_ref,
    geo, chg, ni, nw, cond, in_sem,
    feat, right, wown, woth, back, acc_w, acc_y, keep, total, tile_a, tile_b, flip_a, flip_b,
    xg, xc, xk, ac, sp, sq, pb, rb, sy, ry, sh, rh, s1, s2, s3,
    send_w, recv_w, send_y, recv_y, send_a, recv_a, send_x, recv_x, send_p, recv_p,
    send_b, recv_b, send_m, recv_m, send_h, recv_h, send_t, recv1, recv2, recv3,
):
    row = lax.axis_index("row")
    col = lax.axis_index("col")
    zhigh = row // 8
    place = lax.rem(row, 8)
    chip = place // 2
    core = lax.rem(place, 2)
    yplace = col // 8
    zlow = lax.rem(col, 8)
    zplace = zhigh * 8 + zlow
    up1 = shifted(row, col, 1)
    down1 = shifted(row, col, -1)
    near_dst = shifted(row, col, jnp.where(zlow == 7, 257, 1))
    near_src = shifted(row, col, jnp.where(zlow == 0, -257, -1))
    mate = (lax.rem(row + 8, ROWS), col)
    partner = (zhigh * 8 + chip * 2 + 1 - core, col)
    near_up = zlow != 0
    near_flag = near_up.astype(jnp.int32)
    far = jnp.logical_not(near_up & (place == 0))
    upper_slot = 8 - near_flag
    early = jnp.where(near_up, place + 1, 7 - place)
    late = 8 - early
    lead = jnp.where(near_up, core, 1 - core)
    near_field_early = near_up & (zlow != 7)

    def peer(step):
        return zhigh * 8 + lax.rem(chip + step, 4) * 2 + core, col

    def in_group(step):
        return zhigh * 8 + lax.rem(place + step, 8), col

    def in_y(step):
        return row, lax.rem(yplace + step, 4) * 8 + zlow

    def in_z(step):
        other = lax.rem(zplace + step, 16)
        return (other // 8) * 8 + place, yplace * 8 + lax.rem(other, 8)

    barrier = pltpu.get_barrier_semaphore()
    for other in (mate, near_dst, near_src, up1, down1):
        pl.semaphore_signal(barrier, inc=1, device_id=other, device_id_type=MESH)
    for count, where in ((16, in_z), (4, in_y), (8, in_group)):
        for step in range(1, count):
            pl.semaphore_signal(barrier, inc=1, device_id=where(step), device_id_type=MESH)

    loads = [
        pltpu.make_async_copy(src, dst, in_sem.at[i])
        for i, (src, dst) in enumerate(
            ((geo_in, geo), (chg_in, chg), (ni_in, ni), (nw_in, nw), (cond_in, cond))
        )
    ]
    for load in loads:
        load.start()

    def remote(src, dst, ssem, rsem, where):
        return pltpu.make_async_remote_copy(
            src_ref=src, dst_ref=dst, send_sem=ssem, recv_sem=rsem, device_id=where,
            device_id_type=MESH,
        )

    def w_copies(half):
        lanes = pl.ds(half * WIDTH, WIDTH)
        return [
            remote(
                src.at[:, lanes], dst.at[half], send_w.at[i, half], recv_w.at[i, half], near_dst
            )
            for i, (src, dst) in enumerate(
                zip((geo, chg, cond), (xg.at[7], xc.at[7], xk.at[0]))
            )
        ]

    def y_copies(half):
        return [
            remote(
                ref.at[src, half], ref.at[dst, half], send_y.at[i, half], recv_y.at[i, half], mate
            )
            for i, (ref, src, dst) in enumerate(((xg, 7, 8), (xc, 7, 8), (xk, 0, 1)))
        ]

    copy_a = remote(chg, ac, send_a, recv_a, down1)

    def slot_copies(src, slot, half, where):
        return [
            remote(
                ref.at[src, half], ref.at[slot, half], send_x.at[i, slot, half],
                recv_x.at[i, slot, half], where,
            )
            for i, ref in enumerate((xg, xc))
        ]

    def spread(src, half, upward):
        @pl.when(core == 1 - upward)
        def _():
            for copy in slot_copies(src, 0, half, partner):
                copy.start()

        for step in range(1, 4):

            @pl.when((chip + step < 4) == (upward == 1))
            def _():
                for copy in slot_copies(src, step, half, peer(step)):
                    copy.start()

    def partner_back(step, half):
        return remote(
            sp.at[step, half], pb.at[step, half], send_p.at[step, half], recv_p.at[step, half],
            partner,
        )

    def peer_back(step, half):
        return remote(
            sq.at[step, half], rb.at[step, half], send_b.at[step, half], recv_b.at[step, half],
            peer(4 - step),
        )

    def to_mate(half):
        return remote(sy.at[half], ry.at[half], send_m.at[half], recv_m.at[half], mate)

    def home(half):
        return remote(sh.at[half], rh.at[half], send_h.at[half], recv_h.at[half], near_src)

    for load in loads:
        load.wait()
    own = geo[...]
    feat[...] = jnp.concatenate(features(own)[0], axis=0).T.astype(BF16)
    wown[...] = (chg[...].astype(F32) * (own[3:4] * own[3:4])).astype(BF16)
    pot_ref[...] = jnp.zeros_like(pot_ref)

    def visit(other_geo, other_chg):
        right[...] = jnp.concatenate(features(other_geo)[1], axis=0).astype(BF16)
        woth[...] = (other_chg.astype(F32) * (other_geo[3:4] * other_geo[3:4])).astype(BF16)
        back[...] = jnp.zeros_like(back)
        tiles, flips = (tile_a, tile_b), (flip_a, flip_b)

        def fill(r):
            squared = jnp.dot(
                feat[r * ROWBLK : (r + 1) * ROWBLK, :], right[...], preferred_element_type=F32
            )
            tile = lax.rsqrt(squared).astype(BF16)
            tiles[r % 2][...] = tile
            flips[r % 2][...] = tile.T

        fill(0)
        for r in range(BLOCK // ROWBLK):
            if r + 1 < BLOCK // ROWBLK:
                fill(r + 1)
            rows = slice(r * ROWBLK, (r + 1) * ROWBLK)
            pot_ref[:, rows] += jnp.dot(woth[...], flips[r % 2][...], preferred_element_type=F32)
            back[...] += jnp.dot(wown[:, rows], tiles[r % 2][...], preferred_element_type=F32)

    def own_half(half):
        lanes = pl.ds(pl.multiple_of(half * WIDTH, WIDTH), WIDTH)
        visit(geo[:, lanes], chg[:, lanes])

    own_half(0)
    pl.semaphore_wait(barrier, 30)
    for half in range(CHUNKS):
        for copy in w_copies(half):
            copy.start()
    copy_a.start()
    for half in range(CHUNKS):
        if half + 1 < CHUNKS:
            own_half(half + 1)
        for copy in w_copies(half):
            copy.wait_recv()

        @pl.when(far)
        def _():
            for copy in y_copies(half):
                copy.start()

        spread(7, half, near_flag)

    def near_group(g, carry):
        index = ni[pl.ds(g, 1), :]
        lane = lax.broadcasted_iota(jnp.int32, (1, 128), 1)
        index = jnp.where(lane < nc_ref[g], index, -1)
        slot = lax.broadcasted_iota(jnp.int32, (WIDTH, 128), 0)
        taken = jnp.zeros((RHS, 128), F32)
        sources = [xc[upper_slot, c] for c in range(CHUNKS)]
        for ref in (chg, ac):
            sources += [ref[:, c * WIDTH : (c + 1) * WIDTH] for c in range(CHUNKS)]
        for part, source in enumerate(sources):
            pick = jnp.where(slot == index - part * WIDTH, 1.0, 0.0).astype(BF16)
            taken = taken + jnp.dot(source, pick, preferred_element_type=F32)
        columns = pl.ds(pl.multiple_of(g * 128, 128), 128)
        pot_ref[:, columns] += lax.dot_general(
            taken.astype(BF16), nw[g], NT, preferred_element_type=F32
        )
        return carry

    def near_field():
        copy_a.wait_recv()
        lax.fori_loop(0, GROUPS, near_group, 0)

    pl.when(near_field_early)(near_field)

    def slot_of(t):
        rest = t - CHUNKS * early
        is_late = rest >= 0
        turn = sum((rest >= c * late).astype(jnp.int32) for c in range(1, CHUNKS))
        index = jnp.where(is_late, early + rest - turn * late, t // CHUNKS)
        half = jnp.where(is_late, turn, lax.rem(t, CHUNKS))
        index = index - near_flag
        k = index - lead
        dist = jnp.where(near_up, k // 2 + 1, 3 - k // 2)
        slot = jnp.where((k < 0) | (k == 6), 0, dist + 3 * lax.rem(k + 2, 2))
        return jnp.where((index < 0) | (index == 7), upper_slot, slot), half

    def gather(t, wanted):
        slot, half = slot_of(jnp.maximum(t, 0))

        @pl.when(wanted & (t >= 0) & (slot >= 1) & (slot <= 3))
        def _():
            partner_back(slot, half).wait_recv()
            sq[slot, half] = (keep[slot, half] + pb[slot, half].astype(F32)).astype(BF16)
            peer_back(slot, half).start()

    def is_early(t):
        return t < CHUNKS * early

    def collect(dst, half, upward):
        dst[half] = keep[0, half] * upward.astype(F32)

        @pl.when(core == 1 - upward)
        def _():
            partner_back(0, half).wait_recv()
            dst[half] += pb[0, half].astype(F32)

        for step in range(1, 4):

            @pl.when((chip + step < 4) == (upward == 1))
            def _():
                peer_back(step, half).wait_recv()
                dst[half] += rb[step, half].astype(F32)

    def far_sum(half):
        collect(acc_y, half, 1 - near_flag)
        sy[half] = acc_y[half].astype(BF16)
        to_mate(half).start()

    def step_(t, carry):
        for half in range(CHUNKS):
            at = jnp.minimum(PASS_ON[half], CHUNKS * early + half * late)

            @pl.when((t == at) & far)
            def _():
                for copy in y_copies(half):
                    copy.wait_recv()
                spread(8, half, 1 - near_flag)

        slot, half = slot_of(t)
        direct = (slot >= 1) & (slot <= 3)

        @pl.when(slot < 7)
        def _():
            for copy in slot_copies(7, slot, half, partner):
                copy.wait_recv()

        @pl.when(direct)
        def _():
            for copy in slot_copies(slot, slot + 3, half, partner):
                copy.start()

        visit(xg[slot, half], xc[slot, half])

        @pl.when(direct)
        def _():
            keep[slot, half] = back[...]

        @pl.when(slot >= 7)
        def _():
            keep[0, half] = back[...]

        @pl.when((slot == 0) | ((slot >= 4) & (slot <= 6)))
        def _():
            step = jnp.where(slot == 0, 0, slot - 3)
            sp[step, half] = back[...].astype(BF16)
            partner_back(step, half).start()

        @pl.when((t == jnp.minimum(CHUNKS * early + late + FIRST_HOME, STEPS - 1)) & far)
        def _():
            far_sum(0)

        gather(t - 2 * CHUNKS, is_early(t - 2 * CHUNKS))
        gather(t - 4, jnp.logical_not(is_early(t - 4)))
        return carry

    lax.fori_loop(0, STEPS, step_, 0)

    def tail(t, carry):
        gather(t, is_early(t) | (t >= STEPS - 4))
        return carry

    lax.fori_loop(STEPS - 2 * CHUNKS, STEPS, tail, 0)
    pl.when(jnp.logical_not(near_field_early))(near_field)
    total[...] = member_totals(pot_ref[...], own[3:4], cond[...])

    def near_sum(half, carry):
        collect(acc_w, half, near_flag)
        total[...] += member_totals(acc_w[half], xg[7, half][3:4], xk[0, half])
        return carry

    lax.fori_loop(0, CHUNKS, near_sum, 0)

    @pl.when(far)
    def _():
        total[...] += member_totals(acc_y[0], xg[8, 0][3:4], xk[1, 0])
        far_sum(1)
        total[...] += member_totals(acc_y[1], xg[8, 1][3:4], xk[1, 1])

    local = total[...]
    value = jnp.concatenate([local[q * 8 : q * 8 + 8] for q in range(4)], axis=1)
    sent = 0
    total_copies = []
    for count, mine, where, slots, recv in (
        (8, place, in_group, s1, recv1),
        (4, yplace, in_y, s2, recv2),
        (16, zplace, in_z, s3, recv3),
    ):
        slots[mine] = value
        stage = []
        for step in range(1, count):
            stage.append(
                remote(slots.at[mine], slots.at[mine], send_t.at[sent], recv.at[step], where(step))
            )
            sent += 1
        for copy in stage:
            copy.start()
        if count == 16:
            for half in range(CHUNKS):

                @pl.when(far)
                def _():
                    to_mate(half).wait_recv()
                    acc_w[half] += ry[half].astype(F32)

                sh[half] = acc_w[half].astype(BF16)
                home(half).start()
        for copy in stage:
            copy.wait_recv()
        value = slots[0]
        for other in range(1, count):
            value = value + slots[other]
        total_copies += stage
    for q in range(4):
        tot_ref[q * 8 : q * 8 + 8, :] = value[:, q * RHS : (q + 1) * RHS]

    for half in range(CHUNKS):
        lanes = slice(half * WIDTH, (half + 1) * WIDTH)
        home(half).wait_recv()
        pot_ref[:, lanes] += rh[half].astype(F32)

    copy_a.wait_send()
    for copy in total_copies:
        copy.wait_send()

    def drain(half, carry):
        for copy in w_copies(half):
            copy.wait_send()
        home(half).wait_send()

        @pl.when(far)
        def _():
            for copy in y_copies(half):
                copy.wait_send()
            to_mate(half).wait_send()

        for slot in range(7):
            for copy in slot_copies(7, slot, half, partner):
                copy.wait_send()
        for step in range(4):
            partner_back(step, half).wait_send()
        for step in range(1, 4):
            peer_back(step, half).wait_send()
        return carry

    lax.fori_loop(0, CHUNKS, drain, 0)


def on_device(geometry, charges, near_index, near_count, near_weight, conductor):
    def half(kind, *lead, rows=RHS):
        return pltpu.VMEM((*lead, CHUNKS, rows, WIDTH), kind)

    dma = pltpu.SemaphoreType.DMA
    potential, totals = pl.pallas_call(
        kernel,
        out_shape=(
            jax.ShapeDtypeStruct((RHS, BLOCK), F32),
            jax.ShapeDtypeStruct((RHS, RHS), F32),
        ),
        in_specs=[HBM, HBM, HBM, SMEM, HBM, HBM],
        out_specs=(VMEM, VMEM),
        scratch_shapes=[
            pltpu.VMEM((4, BLOCK), F32), pltpu.VMEM((RHS, BLOCK), BF16),
            pltpu.VMEM((GROUPS, 128), jnp.int32), pltpu.VMEM((GROUPS, 128, 128), BF16),
            pltpu.VMEM((1, BLOCK), jnp.int32), dma((5,)),
            pltpu.VMEM((BLOCK, 40), BF16), pltpu.VMEM((40, WIDTH), BF16),
            pltpu.VMEM((RHS, BLOCK), BF16), pltpu.VMEM((RHS, WIDTH), BF16),
            pltpu.VMEM((RHS, WIDTH), F32), half(F32), half(F32), half(F32, 4), pltpu.VMEM((RHS, RHS), F32),
            *[pltpu.VMEM((ROWBLK, WIDTH), BF16)] * 2, *[pltpu.VMEM((WIDTH, ROWBLK), BF16)] * 2,
            half(F32, 9, rows=4), half(BF16, 9), half(jnp.int32, 2, rows=1),
            pltpu.VMEM((RHS, BLOCK), BF16), half(BF16, 4), half(BF16, 4), half(BF16, 4),
            half(BF16, 4), half(BF16), half(BF16), half(BF16), half(BF16),
            pltpu.VMEM((8, 8, 128), F32), pltpu.VMEM((4, 8, 128), F32),
            pltpu.VMEM((16, 8, 128), F32),
            *[dma((3, CHUNKS))] * 4, dma, dma, *[dma((2, 7, CHUNKS))] * 2,
            *[dma((4, CHUNKS))] * 4, *[dma((CHUNKS,))] * 4, dma((25,)), dma((8,)), dma((4,)),
            dma((16,)),
        ],
        compiler_params=pltpu.CompilerParams(
            collective_id=0, has_side_effects=True, vmem_limit_bytes=VMEM_BYTES
        ),
        name="potential",
    )(geometry, charges, near_index, near_count, near_weight, conductor.reshape(1, BLOCK))
    return potential, totals


def solution(mesh):
    in_specs = (
        P(None, ("row", "col")),
        P(None, ("row", "col")),
        P(("row", "col"), None),
        P(("row", "col")),
        P(("row", "col"), None, None),
        P(("row", "col")),
    )
    out_specs = (P(None, ("row", "col")), P())
    return jax.shard_map(
        on_device, mesh=mesh, in_specs=in_specs, out_specs=out_specs, check_vma=False
    )
```

```python
import jax
import jax.numpy as jnp
from jax import lax
from jax.experimental import pallas as pl
from jax.experimental.pallas import tpu as pltpu
from jax.sharding import PartitionSpec as P

MESH = pl.DeviceIdType.MESH
BLOCK = 1536
CHUNKS = 2
WIDTH = BLOCK // CHUNKS
RHS = 32
GROUPS = 12
ROWBLK = 384
ROWS = 16
COLS = 32
STEPS = 8 * CHUNKS
PASS_ON = (4, 7)
FIRST_HOME = 4
VMEM_BYTES = 62 * 2**20
F32 = jnp.float32
BF16 = jnp.bfloat16
VMEM = pl.BlockSpec(memory_space=pltpu.VMEM)
SMEM = pl.BlockSpec(memory_space=pltpu.SMEM)
HBM = pl.BlockSpec(memory_space=pltpu.HBM)
NT = (((1,), (1,)), ((), ()))


def three(v):
    high = v.astype(BF16).astype(F32)
    rest = v - high
    mid = rest.astype(BF16).astype(F32)
    return high, mid, rest - mid


def features(geo):
    high, mid, low = three(geo[0:3])
    norm = (
        geo[0:1] * geo[0:1] + geo[1:2] * geo[1:2] + geo[2:3] * geo[2:3] + geo[3:4] * geo[3:4]
    )
    nh, nm, nl = three(norm)
    one = jnp.ones_like(norm)
    pad = jnp.zeros((7, geo.shape[1]), F32)
    left = [high, high, high, mid, mid, mid, low, low, low, nh, nm, nl, one, one, one, pad]
    h2, m2, l2 = -2.0 * high, -2.0 * mid, -2.0 * low
    right = [h2, m2, l2, h2, m2, l2, h2, m2, l2, one, one, one, nh, nm, nl, pad]
    return left, right


def shifted(row, col, steps):
    flat = lax.rem(row * COLS + col + (steps + 2 * ROWS * COLS), ROWS * COLS)
    return flat // COLS, lax.rem(flat, COLS)


def member_totals(value, size, conductor):
    pieces = three(value * (size * size))
    slot = lax.broadcasted_iota(jnp.int32, (RHS, value.shape[1]), 0)
    member = jnp.where(slot == conductor, 1.0, 0.0).astype(BF16)
    total = jnp.zeros((RHS, RHS), F32)
    for piece in pieces:
        total = total + lax.dot_general(
            piece.astype(BF16), member, NT, preferred_element_type=F32
        )
    return total


def kernel(
    geo_in, chg_in, ni_in, nc_ref, nw_in, cond_in, pot_ref, tot_ref,
    geo, chg, ni, nw, cond, in_sem,
    feat, right, wown, woth, back, acc_w, acc_y, keep, total, tile_a, tile_b, flip_a, flip_b,
    xg, xc, xk, ac, sp, sq, pb, rb, sy, ry, sh, rh, s1, s2, s3,
    send_w, recv_w, send_y, recv_y, send_a, recv_a, send_x, recv_x, send_p, recv_p,
    send_b, recv_b, send_m, recv_m, send_h, recv_h, send_t, recv1, recv2, recv3,
):
    row = lax.axis_index("row")
    col = lax.axis_index("col")
    zhigh = row // 8
    place = lax.rem(row, 8)
    chip = place // 2
    core = lax.rem(place, 2)
    yplace = col // 8
    zlow = lax.rem(col, 8)
    zplace = zhigh * 8 + zlow
    up1 = shifted(row, col, 1)
    down1 = shifted(row, col, -1)
    near_dst = shifted(row, col, jnp.where(zlow == 7, 257, 1))
    near_src = shifted(row, col, jnp.where(zlow == 0, -257, -1))
    mate = (lax.rem(row + 8, ROWS), col)
    partner = (zhigh * 8 + chip * 2 + 1 - core, col)
    near_up = zlow != 0
    near_flag = near_up.astype(jnp.int32)
    far = jnp.logical_not(near_up & (place == 0))
    upper_slot = 8 - near_flag
    early = jnp.where(near_up, place + 1, 7 - place)
    late = 8 - early
    lead = jnp.where(near_up, core, 1 - core)
    near_field_early = near_up & (zlow != 7)

    def peer(step):
        return zhigh * 8 + lax.rem(chip + step, 4) * 2 + core, col

    def in_group(step):
        return zhigh * 8 + lax.rem(place + step, 8), col

    def in_y(step):
        return row, lax.rem(yplace + step, 4) * 8 + zlow

    def in_z(step):
        other = lax.rem(zplace + step, 16)
        return (other // 8) * 8 + place, yplace * 8 + lax.rem(other, 8)

    barrier = pltpu.get_barrier_semaphore()
    for other in (mate, near_dst, near_src, up1, down1):
        pl.semaphore_signal(barrier, inc=1, device_id=other, device_id_type=MESH)
    for count, where in ((16, in_z), (4, in_y), (8, in_group)):
        for step in range(1, count):
            pl.semaphore_signal(barrier, inc=1, device_id=where(step), device_id_type=MESH)

    loads = [
        pltpu.make_async_copy(src, dst, in_sem.at[i])
        for i, (src, dst) in enumerate(
            ((geo_in, geo), (chg_in, chg), (ni_in, ni), (nw_in, nw), (cond_in, cond))
        )
    ]
    for load in loads:
        load.start()

    def remote(src, dst, ssem, rsem, where):
        return pltpu.make_async_remote_copy(
            src_ref=src, dst_ref=dst, send_sem=ssem, recv_sem=rsem, device_id=where,
            device_id_type=MESH,
        )

    def w_copies(half):
        lanes = pl.ds(half * WIDTH, WIDTH)
        return [
            remote(
                src.at[:, lanes], dst.at[half], send_w.at[i, half], recv_w.at[i, half], near_dst
            )
            for i, (src, dst) in enumerate(
                zip((geo, chg, cond), (xg.at[7], xc.at[7], xk.at[0]))
            )
        ]

    def y_copies(half):
        return [
            remote(
                ref.at[src, half], ref.at[dst, half], send_y.at[i, half], recv_y.at[i, half], mate
            )
            for i, (ref, src, dst) in enumerate(((xg, 7, 8), (xc, 7, 8), (xk, 0, 1)))
        ]

    copy_a = remote(chg, ac, send_a, recv_a, down1)

    def slot_copies(src, slot, half, where):
        return [
            remote(
                ref.at[src, half], ref.at[slot, half], send_x.at[i, slot, half],
                recv_x.at[i, slot, half], where,
            )
            for i, ref in enumerate((xg, xc))
        ]

    def spread(src, half, upward):
        @pl.when(core == 1 - upward)
        def _():
            for copy in slot_copies(src, 0, half, partner):
                copy.start()

        for step in range(1, 4):

            @pl.when((chip + step < 4) == (upward == 1))
            def _():
                for copy in slot_copies(src, step, half, peer(step)):
                    copy.start()

    def partner_back(step, half):
        return remote(
            sp.at[step, half], pb.at[step, half], send_p.at[step, half], recv_p.at[step, half],
            partner,
        )

    def peer_back(step, half):
        return remote(
            sq.at[step, half], rb.at[step, half], send_b.at[step, half], recv_b.at[step, half],
            peer(4 - step),
        )

    def to_mate(half):
        return remote(sy.at[half], ry.at[half], send_m.at[half], recv_m.at[half], mate)

    def home(half):
        return remote(sh.at[half], rh.at[half], send_h.at[half], recv_h.at[half], near_src)

    for load in loads:
        load.wait()
    own = geo[...]
    feat[...] = jnp.concatenate(features(own)[0], axis=0).T.astype(BF16)
    wown[...] = (chg[...].astype(F32) * (own[3:4] * own[3:4])).astype(BF16)
    pot_ref[...] = jnp.zeros_like(pot_ref)

    def visit(other_geo, other_chg):
        right[...] = jnp.concatenate(features(other_geo)[1], axis=0).astype(BF16)
        woth[...] = (other_chg.astype(F32) * (other_geo[3:4] * other_geo[3:4])).astype(BF16)
        back[...] = jnp.zeros_like(back)
        tiles, flips = (tile_a, tile_b), (flip_a, flip_b)

        def fill(r):
            squared = jnp.dot(
                feat[r * ROWBLK : (r + 1) * ROWBLK, :], right[...], preferred_element_type=F32
            )
            tile = lax.rsqrt(squared).astype(BF16)
            tiles[r % 2][...] = tile
            flips[r % 2][...] = tile.T

        fill(0)
        for r in range(BLOCK // ROWBLK):
            if r + 1 < BLOCK // ROWBLK:
                fill(r + 1)
            rows = slice(r * ROWBLK, (r + 1) * ROWBLK)
            pot_ref[:, rows] += jnp.dot(woth[...], flips[r % 2][...], preferred_element_type=F32)
            back[...] += jnp.dot(wown[:, rows], tiles[r % 2][...], preferred_element_type=F32)

    def own_half(half):
        lanes = pl.ds(pl.multiple_of(half * WIDTH, WIDTH), WIDTH)
        visit(geo[:, lanes], chg[:, lanes])

    own_half(0)
    pl.semaphore_wait(barrier, 30)
    for half in range(CHUNKS):
        for copy in w_copies(half):
            copy.start()
    copy_a.start()
    for half in range(CHUNKS):
        if half + 1 < CHUNKS:
            own_half(half + 1)
        for copy in w_copies(half):
            copy.wait_recv()

        @pl.when(far)
        def _():
            for copy in y_copies(half):
                copy.start()

        spread(7, half, near_flag)

    def near_group(g, carry):
        index = ni[pl.ds(g, 1), :]
        lane = lax.broadcasted_iota(jnp.int32, (1, 128), 1)
        index = jnp.where(lane < nc_ref[g], index, -1)
        slot = lax.broadcasted_iota(jnp.int32, (WIDTH, 128), 0)
        taken = jnp.zeros((RHS, 128), F32)
        sources = [xc[upper_slot, c] for c in range(CHUNKS)]
        for ref in (chg, ac):
            sources += [ref[:, c * WIDTH : (c + 1) * WIDTH] for c in range(CHUNKS)]
        for part, source in enumerate(sources):
            pick = jnp.where(slot == index - part * WIDTH, 1.0, 0.0).astype(BF16)
            taken = taken + jnp.dot(source, pick, preferred_element_type=F32)
        columns = pl.ds(pl.multiple_of(g * 128, 128), 128)
        pot_ref[:, columns] += lax.dot_general(
            taken.astype(BF16), nw[g], NT, preferred_element_type=F32
        )
        return carry

    def near_field():
        copy_a.wait_recv()
        lax.fori_loop(0, GROUPS, near_group, 0)

    pl.when(near_field_early)(near_field)

    def slot_of(t):
        rest = t - CHUNKS * early
        is_late = rest >= 0
        turn = sum((rest >= c * late).astype(jnp.int32) for c in range(1, CHUNKS))
        index = jnp.where(is_late, early + rest - turn * late, t // CHUNKS)
        half = jnp.where(is_late, turn, lax.rem(t, CHUNKS))
        index = index - near_flag
        k = index - lead
        dist = jnp.where(near_up, k // 2 + 1, 3 - k // 2)
        slot = jnp.where((k < 0) | (k == 6), 0, dist + 3 * lax.rem(k + 2, 2))
        return jnp.where((index < 0) | (index == 7), upper_slot, slot), half

    def gather(t, wanted):
        slot, half = slot_of(jnp.maximum(t, 0))

        @pl.when(wanted & (t >= 0) & (slot >= 1) & (slot <= 3))
        def _():
            partner_back(slot, half).wait_recv()
            sq[slot, half] = (keep[slot, half] + pb[slot, half].astype(F32)).astype(BF16)
            peer_back(slot, half).start()

    def is_early(t):
        return t < CHUNKS * early

    def collect(dst, half, upward):
        dst[half] = keep[0, half] * upward.astype(F32)

        @pl.when(core == 1 - upward)
        def _():
            partner_back(0, half).wait_recv()
            dst[half] += pb[0, half].astype(F32)

        for step in range(1, 4):

            @pl.when((chip + step < 4) == (upward == 1))
            def _():
                peer_back(step, half).wait_recv()
                dst[half] += rb[step, half].astype(F32)

    def far_sum(half):
        collect(acc_y, half, 1 - near_flag)
        sy[half] = acc_y[half].astype(BF16)
        to_mate(half).start()

    def step_(t, carry):
        for half in range(CHUNKS):
            at = jnp.minimum(PASS_ON[half], CHUNKS * early + half * late)

            @pl.when((t == at) & far)
            def _():
                for copy in y_copies(half):
                    copy.wait_recv()
                spread(8, half, 1 - near_flag)

        slot, half = slot_of(t)
        direct = (slot >= 1) & (slot <= 3)

        @pl.when(slot < 7)
        def _():
            for copy in slot_copies(7, slot, half, partner):
                copy.wait_recv()

        @pl.when(direct)
        def _():
            for copy in slot_copies(slot, slot + 3, half, partner):
                copy.start()

        visit(xg[slot, half], xc[slot, half])

        @pl.when(direct)
        def _():
            keep[slot, half] = back[...]

        @pl.when(slot >= 7)
        def _():
            keep[0, half] = back[...]

        @pl.when((slot == 0) | ((slot >= 4) & (slot <= 6)))
        def _():
            step = jnp.where(slot == 0, 0, slot - 3)
            sp[step, half] = back[...].astype(BF16)
            partner_back(step, half).start()

        @pl.when((t == jnp.minimum(CHUNKS * early + late + FIRST_HOME, STEPS - 1)) & far)
        def _():
            far_sum(0)

        gather(t - 2 * CHUNKS, is_early(t - 2 * CHUNKS))
        gather(t - 3, jnp.logical_not(is_early(t - 3)))
        return carry

    lax.fori_loop(0, STEPS, step_, 0)

    def tail(t, carry):
        gather(t, is_early(t) | (t >= STEPS - 3))
        return carry

    lax.fori_loop(STEPS - 2 * CHUNKS, STEPS, tail, 0)
    pl.when(jnp.logical_not(near_field_early))(near_field)
    total[...] = member_totals(pot_ref[...], own[3:4], cond[...])

    def near_sum(half, carry):
        collect(acc_w, half, near_flag)
        total[...] += member_totals(acc_w[half], xg[7, half][3:4], xk[0, half])
        return carry

    lax.fori_loop(0, CHUNKS, near_sum, 0)

    @pl.when(far)
    def _():
        total[...] += member_totals(acc_y[0], xg[8, 0][3:4], xk[1, 0])
        far_sum(1)
        total[...] += member_totals(acc_y[1], xg[8, 1][3:4], xk[1, 1])

    local = total[...]
    value = jnp.concatenate([local[q * 8 : q * 8 + 8] for q in range(4)], axis=1)
    sent = 0
    total_copies = []
    for count, mine, where, slots, recv in (
        (8, place, in_group, s1, recv1),
        (4, yplace, in_y, s2, recv2),
        (16, zplace, in_z, s3, recv3),
    ):
        slots[mine] = value
        stage = []
        for step in range(1, count):
            stage.append(
                remote(slots.at[mine], slots.at[mine], send_t.at[sent], recv.at[step], where(step))
            )
            sent += 1
        for copy in stage:
            copy.start()
        if count == 16:
            for half in range(CHUNKS):

                @pl.when(far)
                def _():
                    to_mate(half).wait_recv()
                    acc_w[half] += ry[half].astype(F32)

                sh[half] = acc_w[half].astype(BF16)
                home(half).start()
        for copy in stage:
            copy.wait_recv()
        value = slots[0]
        for other in range(1, count):
            value = value + slots[other]
        total_copies += stage
    for q in range(4):
        tot_ref[q * 8 : q * 8 + 8, :] = value[:, q * RHS : (q + 1) * RHS]

    for half in range(CHUNKS):
        lanes = slice(half * WIDTH, (half + 1) * WIDTH)
        home(half).wait_recv()
        pot_ref[:, lanes] += rh[half].astype(F32)

    copy_a.wait_send()
    for copy in total_copies:
        copy.wait_send()

    def drain(half, carry):
        for copy in w_copies(half):
            copy.wait_send()
        home(half).wait_send()

        @pl.when(far)
        def _():
            for copy in y_copies(half):
                copy.wait_send()
            to_mate(half).wait_send()

        for slot in range(7):
            for copy in slot_copies(7, slot, half, partner):
                copy.wait_send()
        for step in range(4):
            partner_back(step, half).wait_send()
        for step in range(1, 4):
            peer_back(step, half).wait_send()
        return carry

    lax.fori_loop(0, CHUNKS, drain, 0)


def on_device(geometry, charges, near_index, near_count, near_weight, conductor):
    def half(kind, *lead, rows=RHS):
        return pltpu.VMEM((*lead, CHUNKS, rows, WIDTH), kind)

    dma = pltpu.SemaphoreType.DMA
    potential, totals = pl.pallas_call(
        kernel,
        out_shape=(
            jax.ShapeDtypeStruct((RHS, BLOCK), F32),
            jax.ShapeDtypeStruct((RHS, RHS), F32),
        ),
        in_specs=[HBM, HBM, HBM, SMEM, HBM, HBM],
        out_specs=(VMEM, VMEM),
        scratch_shapes=[
            pltpu.VMEM((4, BLOCK), F32), pltpu.VMEM((RHS, BLOCK), BF16),
            pltpu.VMEM((GROUPS, 128), jnp.int32), pltpu.VMEM((GROUPS, 128, 128), BF16),
            pltpu.VMEM((1, BLOCK), jnp.int32), dma((5,)),
            pltpu.VMEM((BLOCK, 40), BF16), pltpu.VMEM((40, WIDTH), BF16),
            pltpu.VMEM((RHS, BLOCK), BF16), pltpu.VMEM((RHS, WIDTH), BF16),
            pltpu.VMEM((RHS, WIDTH), F32), half(F32), half(F32), half(F32, 4), pltpu.VMEM((RHS, RHS), F32),
            *[pltpu.VMEM((ROWBLK, WIDTH), BF16)] * 2, *[pltpu.VMEM((WIDTH, ROWBLK), BF16)] * 2,
            half(F32, 9, rows=4), half(BF16, 9), half(jnp.int32, 2, rows=1),
            pltpu.VMEM((RHS, BLOCK), BF16), half(BF16, 4), half(BF16, 4), half(BF16, 4),
            half(BF16, 4), half(BF16), half(BF16), half(BF16), half(BF16),
            pltpu.VMEM((8, 8, 128), F32), pltpu.VMEM((4, 8, 128), F32),
            pltpu.VMEM((16, 8, 128), F32),
            *[dma((3, CHUNKS))] * 4, dma, dma, *[dma((2, 7, CHUNKS))] * 2,
            *[dma((4, CHUNKS))] * 4, *[dma((CHUNKS,))] * 4, dma((25,)), dma((8,)), dma((4,)),
            dma((16,)),
        ],
        compiler_params=pltpu.CompilerParams(
            collective_id=0, has_side_effects=True, vmem_limit_bytes=VMEM_BYTES
        ),
        name="potential",
    )(geometry, charges, near_index, near_count, near_weight, conductor.reshape(1, BLOCK))
    return potential, totals


def solution(mesh):
    in_specs = (
        P(None, ("row", "col")),
        P(None, ("row", "col")),
        P(("row", "col"), None),
        P(("row", "col")),
        P(("row", "col"), None, None),
        P(("row", "col")),
    )
    out_specs = (P(None, ("row", "col")), P())
    return jax.shard_map(
        on_device, mesh=mesh, in_specs=in_specs, out_specs=out_specs, check_vma=False
    )
```
